256 devices in a mesh: frame: 16 (over x_hi, z), height: 8 (over x_lo, y), dp: 2 (over core).
Axes of the slice: x: 4 (x_hi: 2, x_lo: 2; x = x_hi * 2 + x_lo), y: 4, z: 8, core: 2. Of those that a mesh axis runs over, the one named last changes fastest.
Arguments:
- clip_latents: bfloat16 [2, 32, 128, 16, 320], P('dp', 'frame', 'height'), may hold values from -6 to 6
- out_grad: bfloat16 [2, 32, 128, 16, 320], P('dp', 'frame', 'height'), may hold values from -6 to 6
- box_mask: int32 [2, 32, 128, 16], P('dp', 'frame', 'height'), may hold values from 0 to 1, as said below
- attn_weights: bfloat16 [1280, 320], replicated, may hold values from -0.3125 to 0.3125
- conv_weights: bfloat16 [2880, 320], replicated, may hold values from -0.109375 to 0.109375
- time_bias: float32 [5, 32, 32], replicated, may hold values from -4 to 250
Outputs:
- grad_input: bfloat16 [2, 32, 128, 16, 320], P('dp', 'frame', 'height')
- grad_attn: float32 [1280, 320], P(('frame', 'height', 'dp'))
- grad_conv: float32 [2880, 320], P(('height', 'dp'))
The draws below stay inside these ranges and needn't reach their ends.
Inputs may be any that keep to these rules, and one draw needn't show every extreme that they name: Each frame of each clip has one grounding box: box_mask is 1 on a rectangle of 32 to 64 rows and 4 to 8 columns, 0 elsewhere.
All inputs are finite; a program needn't handle non-finite values.
Results may differ from the reference program's by a relative error of at most 0.025.
Values may be sent and summed in bfloat16 or wider, within the bound.
A program may use at most 64 MiB of HBM per device.

```python
import jax
import jax.numpy as jnp
from jax import lax

HEADS = 5
C = 320
WID = 16
CLIPS = 2
FRAMES = 32
HGT = 128


def draw_box_mask(key, part):
    keys = jax.random.split(jax.random.fold_in(key, 11), 4)
    shape = (CLIPS, FRAMES)
    box_top = jax.random.randint(keys[0], shape, 0, HGT // 2)
    box_tall = jax.random.randint(keys[1], shape, HGT // 4, HGT // 2 + 1)
    box_left = jax.random.randint(keys[2], shape, 0, WID // 2)
    box_wide = jax.random.randint(keys[3], shape, WID // 4, WID // 2 + 1)
    row_ids = jnp.arange(HGT)[None, None, :]
    col_ids = jnp.arange(WID)[None, None, :]
    inside_rows = (row_ids >= box_top[..., None]) & (row_ids < (box_top + box_tall)[..., None])
    inside_cols = (col_ids >= box_left[..., None]) & (col_ids < (box_left + box_wide)[..., None])
    inside = inside_rows[..., :, None] & inside_cols[..., None, :]
    return inside.astype(jnp.int32)


def draw_time_bias(key, part):
    keys = jax.random.split(jax.random.fold_in(key, 23), 1)
    shape = (HEADS, FRAMES, FRAMES)
    values = jnp.clip(jax.random.normal(keys[0], shape, jnp.float32), -4.0, 4.0)
    return values.astype(jnp.float32)


def shard_levels(stream_key, dims, cuts, least, largest):
    loudness = 1.0
    for axis_at, blocks in cuts:
        draws = jax.random.uniform(jax.random.fold_in(jax.random.fold_in(stream_key, 6), axis_at), (blocks,), jnp.float32, least / len(cuts), largest / len(cuts))
        loudness = loudness * jnp.repeat(jnp.exp(draws), dims[axis_at] // blocks).reshape((-1,) + (1,) * (len(dims) - 1 - axis_at))
    return loudness


def bell_draw(rng, dims, width, limit, shards=(), dtype=jnp.bfloat16):
    gain = shard_levels(rng, dims, shards, -0.22, 0.18) if shards else 1.0
    array = jax.random.normal(rng, dims, jnp.float32) * width * gain
    return jnp.minimum(jnp.maximum(array, -limit), limit).astype(dtype)


def setup_inputs(seed: int = 0) -> dict:
    splits = jax.random.split(jax.random.key(seed), 7)
    clip_latents = bell_draw(splits[0], (CLIPS, FRAMES, HGT, WID, C), 1.0, 6.0, ((0, 2), (1, 16), (2, 8)))
    out_grad = bell_draw(splits[1], (CLIPS, FRAMES, HGT, WID, C), 1.0, 6.0, ((0, 2), (1, 16), (2, 8)))
    box_mask = draw_box_mask(jax.random.fold_in(splits[6], 71), 0)
    attn_weights = bell_draw(splits[3], (4 * C, C), C ** -0.5, 0.3125)
    conv_weights = bell_draw(splits[4], (9 * C, C), (9 * C) ** -0.5, 0.109375)
    time_bias = draw_time_bias(jax.random.fold_in(splits[6], 71), 0)
    return {"clip_latents": clip_latents, "out_grad": out_grad, "box_mask": box_mask, "attn_weights": attn_weights, "conv_weights": conv_weights, "time_bias": time_bias}


ground_bias = 2.0


def silu_slope(value):
    sig = jax.nn.sigmoid(value)
    return sig * (1.0 + value * (1.0 - sig))


def matmul(left, right):
    return jnp.dot(left, right, preferred_element_type=jnp.float32)


def one_clip(inputs, attn_weights, conv_weights, time_bias):
    latents, upstream_grad, marks = inputs
    frame_count, row_count, col_count, channels = latents.shape
    pixels = row_count * col_count
    head_size = channels // HEADS
    scaling = head_size ** -0.5
    w_query = attn_weights[:channels]
    w_key = attn_weights[channels:2 * channels]
    w_value = attn_weights[2 * channels:3 * channels]
    w_out = attn_weights[3 * channels:]
    flat_x = latents.reshape(-1, channels)
    query_rows = matmul(flat_x, w_query).astype(jnp.bfloat16)
    key_rows = matmul(flat_x, w_key).astype(jnp.bfloat16)
    value_rows = matmul(flat_x, w_value).astype(jnp.bfloat16)
    head_shape = (frame_count, pixels, HEADS, head_size)
    qh = query_rows.reshape(head_shape).astype(jnp.float32)
    kh = key_rows.reshape(head_shape).astype(jnp.float32)
    vh = value_rows.reshape(head_shape).astype(jnp.float32)
    mark_bias = ground_bias * marks.reshape(frame_count, pixels).T.astype(jnp.float32)
    scores = jnp.einsum("tnhd,unhd->nhtu", qh, kh) * scaling + time_bias[None] + mark_bias[:, None, None, :]
    prob_full = jax.nn.softmax(scores, axis=-1)
    prob_half = prob_full.astype(jnp.bfloat16)
    mixed_rows = jnp.einsum("nhtu,unhd->tnhd", prob_half.astype(jnp.float32), vh).astype(jnp.bfloat16).reshape(-1, channels)
    residual = (flat_x.astype(jnp.float32) + matmul(mixed_rows, w_out)).astype(jnp.bfloat16)
    activated = jax.nn.silu(residual.astype(jnp.float32)).astype(jnp.bfloat16)
    image_shape = (frame_count, row_count, col_count, channels)
    widths = ((0, 0), (1, 1), (1, 1), (0, 0))
    act_pad = jnp.pad(activated.reshape(image_shape), widths)
    grad_pad = jnp.pad(upstream_grad, widths)
    out_rows = upstream_grad.reshape(-1, channels)
    delta_sum = jnp.zeros((frame_count * pixels, channels), jnp.float32)
    conv_terms = []
    for row_step in (-1, 0, 1):
        for col_step in (-1, 0, 1):
            tap_index = 3 * (row_step + 1) + col_step + 1
            tap_weight = conv_weights[tap_index * channels:(tap_index + 1) * channels]
            shifted = grad_pad[:, 1 - row_step:1 - row_step + row_count, 1 - col_step:1 - col_step + col_count, :]
            delta_sum = delta_sum + matmul(shifted.reshape(-1, channels), tap_weight.T)
            moved_rows = act_pad[:, 1 + row_step:1 + row_step + row_count, 1 + col_step:1 + col_step + col_count, :]
            conv_terms.append(matmul(moved_rows.reshape(-1, channels).T, out_rows))
    upstream = (out_rows.astype(jnp.float32) + silu_slope(residual.astype(jnp.float32)) * delta_sum).astype(jnp.bfloat16)
    d_mixed = matmul(upstream, w_out.T).astype(jnp.bfloat16)
    dh = d_mixed.reshape(head_shape).astype(jnp.float32)
    d_prob = jnp.einsum("tnhd,unhd->nhtu", dh, vh)
    row_dot = jnp.sum(prob_full * d_prob, axis=-1, keepdims=True)
    d_scores = (prob_full * (d_prob - row_dot)).astype(jnp.bfloat16).astype(jnp.float32)
    d_query = (jnp.einsum("nhtu,unhd->tnhd", d_scores, kh) * scaling).astype(jnp.bfloat16).reshape(-1, channels)
    d_key = (jnp.einsum("nhtu,tnhd->unhd", d_scores, qh) * scaling).astype(jnp.bfloat16).reshape(-1, channels)
    d_value = jnp.einsum("nhtu,tnhd->unhd", prob_half.astype(jnp.float32), dh).astype(jnp.bfloat16).reshape(-1, channels)
    d_inputs = (matmul(d_query, w_query.T) + matmul(d_key, w_key.T) + matmul(d_value, w_value.T)).astype(jnp.bfloat16)
    grad_rows = (upstream.astype(jnp.float32) + d_inputs.astype(jnp.float32)).astype(jnp.bfloat16)
    attn_term = jnp.concatenate([matmul(flat_x.T, d_query), matmul(flat_x.T, d_key), matmul(flat_x.T, d_value), matmul(mixed_rows.T, upstream)], axis=0)
    conv_term = jnp.concatenate(conv_terms, axis=0)
    return grad_rows.reshape(image_shape), attn_term, conv_term


def reference(clip_latents, out_grad, box_mask, attn_weights, conv_weights, time_bias):
    grad_input, attn_terms, conv_terms = lax.map(
        lambda inputs: one_clip(inputs, attn_weights, conv_weights, time_bias),
        (clip_latents, out_grad, box_mask))
    grad_scale = (CLIPS * FRAMES * HGT * WID) ** -0.5
    grad_attn = jnp.sum(attn_terms, axis=0) * grad_scale
    grad_conv = jnp.sum(conv_terms, axis=0) * grad_scale
    return grad_input, grad_attn, grad_conv
```

```python
import jax
import jax.numpy as jnp
from jax import lax
from jax.experimental import pallas as pl
from jax.experimental.pallas import tpu as pltpu
from jax.sharding import PartitionSpec as P

F32 = jnp.float32
BF16 = jnp.bfloat16
GROUND_BIAS = 2.0
NF, NH, ND = 16, 8, 2
C = 320
CP = 384
HEADS = 5
T = 32
W = 16
ROWS = T * W
BLK = 128
NB = ROWS // BLK
NEG = -1e30
TOKENS = 2 * 32 * 128 * 16
GRAD_SCALE = float(TOKENS) ** -0.5
SCALING = 0.125


def peer(**where):
    return dict(device_id=where, device_id_type=pl.DeviceIdType.MESH)


def gather_kernel(x_ref, dy_ref, xt_ref, dy0_ref, dyu_ref, dyd_ref, xs, xr, ds, dr, hs, hr, ls):
    f = lax.axis_index("frame")
    h = lax.axis_index("height")
    lin = h * NF + f
    prev = lax.rem(lin + NF * NH - 1, NF * NH)
    nxt = lax.rem(lin + 1, NF * NH)
    barrier = pltpu.get_barrier_semaphore()
    for k in range(1, NF):
        pl.semaphore_signal(barrier, inc=1, **peer(frame=lax.rem(f + k, NF)))

    @pl.when(f == 0)
    def _():
        pl.semaphore_signal(barrier, inc=1, **peer(frame=lax.rem(prev, NF), height=prev // NF))

    @pl.when(f == NF - 1)
    def _():
        pl.semaphore_signal(barrier, inc=1, **peer(frame=lax.rem(nxt, NF), height=nxt // NF))

    edge = jnp.where(jnp.logical_or(f == 0, f == NF - 1), 1, 0)
    pl.semaphore_wait(barrier, NF - 1 + edge)

    def sends(src, dst, ssem, rsem):
        out = []
        for k in range(1, NF):
            p = lax.rem(f + k, NF)
            cp = pltpu.make_async_remote_copy(
                src_ref=src.at[:, p],
                dst_ref=dst.at[pl.ds(2 * f, 2)],
                send_sem=ssem.at[k],
                recv_sem=rsem.at[k],
                **peer(frame=p),
            )
            cp.start()
            out.append(cp)
        return out

    xc = sends(x_ref, xt_ref, xs, xr)
    dc = sends(dy_ref, dy0_ref, ds, dr)
    lx = pltpu.make_async_copy(x_ref.at[:, f], xt_ref.at[pl.ds(2 * f, 2)], ls.at[0])
    ld = pltpu.make_async_copy(dy_ref.at[:, f], dy0_ref.at[pl.ds(2 * f, 2)], ls.at[1])
    lx.start()
    ld.start()
    lx.wait()
    ld.wait()
    for cp in xc:
        cp.wait_recv()
    for cp in dc:
        cp.wait_recv()
    up = pltpu.make_async_remote_copy(
        src_ref=dy0_ref,
        dst_ref=dyd_ref,
        send_sem=hs.at[0],
        recv_sem=hr.at[0],
        **peer(frame=lax.rem(prev, NF), height=prev // NF),
    )
    down = pltpu.make_async_remote_copy(
        src_ref=dy0_ref,
        dst_ref=dyu_ref,
        send_sem=hs.at[1],
        recv_sem=hr.at[1],
        **peer(frame=lax.rem(nxt, NF), height=nxt // NF),
    )
    up.start()
    down.start()
    for cp in xc + dc:
        cp.wait_send()
    up.wait()
    down.wait()


def gather_rows(x_aug, dy):
    vm = pl.BlockSpec(memory_space=pltpu.VMEM)
    row = jax.ShapeDtypeStruct((T, W, C), BF16)
    dma = pltpu.SemaphoreType.DMA
    return pl.pallas_call(
        gather_kernel,
        out_shape=(jax.ShapeDtypeStruct((T, W, CP), BF16), row, row, row),
        in_specs=[vm, vm],
        out_specs=(vm, vm, vm, vm),
        scratch_shapes=[dma((NF,)), dma((NF,)), dma((NF,)), dma((NF,)), dma((2,)), dma((2,)), dma((2,))],
        compiler_params=pltpu.CompilerParams(collective_id=0, has_side_effects=True),
        name="gather_rows",
    )(x_aug, dy)


def nn(a, b):
    return lax.dot_general(a, b, (((1,), (0,)), ((), ())), preferred_element_type=F32)


def nt(a, b):
    return lax.dot_general(a, b, (((1,), (1,)), ((), ())), preferred_element_type=F32)


def tn(a, b):
    return lax.dot_general(a, b, (((0,), (0,)), ((), ())), preferred_element_type=F32)


def pixel_major(src, tr, store, width):
    for s in range(0, width, 128):
        w = min(128, width - s)
        tr[s // 128, :, :w] = src[:, :, s : s + w].reshape(ROWS, w).astype(F32)
    for p in range(W):
        for s in range(0, width, 128):
            w = min(128, width - s)
            store(p, s, w, tr[s // 128, pl.ds(p, T, stride=W), :][:, :w].astype(BF16))


def compute_kernel(
    xt_ref, dy0_ref, dyu_ref, dyd_ref, wa_ref, wc_ref, tb_ref,
    gi_ref, attn_ref, conv_ref,
    tr, xp, dyp, q_s, k_s, v_s, o_s, pr, bias_s, y1_s, a_t, da_s, g_s, do_s, dq_s, dk_s, dv_s, x_t, o_t, cf,
):
    lin = lax.axis_index("height") * NF + lax.axis_index("frame")

    def put_x(p, s, w, val):
        xp[p * T : (p + 1) * T, s : s + w] = val

    pixel_major(xt_ref, tr, put_x, CP)
    x = xp[:, :C]
    q_s[...] = nn(x, wa_ref[0:C]).astype(BF16)
    k_s[...] = nn(x, wa_ref[C : 2 * C]).astype(BF16)
    v_s[...] = nn(x, wa_ref[2 * C : 3 * C]).astype(BF16)

    ri = lax.broadcasted_iota(jnp.int32, (BLK, BLK), 0) // T
    ci = lax.broadcasted_iota(jnp.int32, (BLK, BLK), 1) // T
    for hd in range(HEADS):
        one = tb_ref[hd]
        wide = jnp.concatenate([one] * 4, axis=1)
        full = jnp.concatenate([wide] * 4, axis=0)
        bias_s[hd] = jnp.where(ri == ci, full, NEG)
    lane = lax.broadcasted_iota(jnp.int32, (BLK, 128), 1)
    low = lane < 64
    ones = jnp.full((8, 128), GROUND_BIAS, BF16)

    slabs = ((0, 128, (0, 1)), (128, 128, (2, 3)), (256, 64, (4,)))

    def only(val, i, w):
        if w == 64:
            return val
        keep = low if i == 0 else jnp.logical_not(low)
        return jnp.where(keep, val, jnp.zeros_like(val))

    def pick(parts, w):
        if w == 64:
            return parts[0]
        return jnp.where(low, parts[0], parts[1])

    for b in range(NB):
        rows = slice(b * BLK, (b + 1) * BLK)
        marks = jnp.where(lane == 64, xp[rows, 256:384], jnp.zeros((BLK, 128), BF16))
        key_bias = nt(ones, marks)[0:1, :]
        for s, w, heads in slabs:
            ls = slice(s, s + w)
            qb, kb, vb = q_s[rows, ls], k_s[rows, ls], v_s[rows, ls]
            outs = []
            for i, hd in enumerate(heads):
                sc = nt(only(qb, i, w), kb) * SCALING + bias_s[hd] + key_bias
                e = jnp.exp(sc - jnp.max(sc, axis=-1, keepdims=True))
                pf = e / jnp.sum(e, axis=-1, keepdims=True)
                pr[b, hd] = pf
                outs.append(nn(pf.astype(BF16), vb))
            o_s[rows, ls] = pick(outs, w).astype(BF16)

    y1 = (x.astype(F32) + nn(o_s[...], wa_ref[3 * C :])).astype(BF16)
    y1_s[...] = y1
    yf = y1.astype(F32)
    act = yf / (1.0 + jnp.exp(-yf))
    a_t[...] = act.T.astype(BF16)
    x_t[...] = x.astype(F32).T.astype(BF16)
    o_t[...] = o_s[...].astype(F32).T.astype(BF16)

    zero = jnp.zeros((T, C), BF16)
    for r, (src, keep) in enumerate(((dyd_ref, lin < NF * NH - 1), (dy0_ref, None), (dyu_ref, lin > 0))):
        dyp[r, 0:T, :] = zero
        dyp[r, (W + 1) * T :, :] = zero

        def put(p, s, w, val, r=r, keep=keep):
            if keep is not None:
                val = jnp.where(keep, val, jnp.zeros_like(val))
            dyp[r, (p + 1) * T : (p + 2) * T, s : s + w] = val

        pixel_major(src, tr, put, C)

    first = True
    for r in range(3):
        for c in range(3):
            tap = 3 * r + c
            off = (2 - c) * T
            shifted = dyp[r, off : off + ROWS, :]
            taps = slice(tap * C, (tap + 1) * C)
            part = nt(shifted, wc_ref[taps])
            da_s[...] = part if first else da_s[...] + part
            first = False
            cf[taps, :] = nn(a_t[...], shifted) * GRAD_SCALE
    for k in range(NH * ND):
        conv_ref[k // ND, k % ND] = cf[k * 180 : (k + 1) * 180, :].astype(BF16)

    yf = y1_s[...].astype(F32)
    sig = 1.0 / (1.0 + jnp.exp(-yf))
    slope = sig * (1.0 + yf * (1.0 - sig))
    g = (dyp[1, T : T + ROWS, :].astype(F32) + slope * da_s[...]).astype(BF16)
    g_s[...] = g
    do_s[...] = nt(g, wa_ref[3 * C :]).astype(BF16)

    for b in range(NB):
        rows = slice(b * BLK, (b + 1) * BLK)
        for s, w, heads in slabs:
            ls = slice(s, s + w)
            qb, kb, vb, db = q_s[rows, ls], k_s[rows, ls], v_s[rows, ls], do_s[rows, ls]
            dqs, dks, dvs = [], [], []
            for i, hd in enumerate(heads):
                pf = pr[b, hd]
                dp = nt(only(db, i, w), vb)
                dsc = (pf * (dp - jnp.sum(pf * dp, axis=-1, keepdims=True)))
                dsc = dsc.astype(BF16)
                dqs.append(nn(dsc, kb))
                dks.append(tn(dsc, qb))
                dvs.append(tn(pf.astype(BF16), db))
            dq_s[rows, ls] = (pick(dqs, w) * SCALING).astype(BF16)
            dk_s[rows, ls] = (pick(dks, w) * SCALING).astype(BF16)
            dv_s[rows, ls] = pick(dvs, w).astype(BF16)

    dx = nt(dq_s[...], wa_ref[0:C]) + nt(dk_s[...], wa_ref[C : 2 * C]) + nt(dv_s[...], wa_ref[2 * C : 3 * C])
    gi = g_s[...].astype(F32) + dx.astype(BF16).astype(F32)
    for s in range(0, C, 128):
        w = min(128, C - s)
        tr[s // 128, :, :w] = gi[:, s : s + w]
    for t in range(T):
        for s in range(0, C, 128):
            w = min(128, C - s)
            gi_ref[t, :, s : s + w] = tr[s // 128, pl.ds(t, W, stride=T), :][:, :w].astype(BF16)

    for j, (left, right) in enumerate(((x_t, dq_s), (x_t, dk_s), (x_t, dv_s), (o_t, g_s))):
        term = (nn(left[...], right[...]) * GRAD_SCALE).astype(F32)
        for k in range(8):
            m = 8 * j + k
            attn_ref[m // 2, m % 2] = term[40 * k : 40 * (k + 1), :].astype(BF16)


def compute(xt, dy0, dyu, dyd, wa, wc, tb):
    vm = pl.BlockSpec(memory_space=pltpu.VMEM)
    v = pltpu.VMEM
    tok = v((ROWS, C), BF16)
    return pl.pallas_call(
        compute_kernel,
        out_shape=(
            jax.ShapeDtypeStruct((T, W, C), BF16),
            jax.ShapeDtypeStruct((NF, ND, 40, C), BF16),
            jax.ShapeDtypeStruct((NH, ND, 180, C), BF16),
        ),
        in_specs=[vm] * 7,
        out_specs=(vm, vm, vm),
        scratch_shapes=[
            v((3, ROWS, 128), F32), v((ROWS, CP), BF16), v((3, ROWS + 2 * T, C), BF16),
            tok, tok, tok, tok,
            v((NB, HEADS, BLK, BLK), F32), v((HEADS, BLK, BLK), F32),
            tok, v((C, ROWS), BF16), v((ROWS, C), F32), tok, tok, tok, tok, tok,
            v((C, ROWS), BF16), v((C, ROWS), BF16), v((9 * C, C), F32),
        ],
        name="block_backward",
    )(xt, dy0, dyu, dyd, wa, wc, tb)


def scatter_kernel(
    gi_ref, attn_ref, conv_ref,
    out_ref, oattn_ref, oconv_ref,
    conv_a, attn_a, conv_1, attn_1, conv_b, attn_b, conv_f, conv_c, conv_cr, conv_d, conv_dr, attn_c, attn_cr,
    gs, gr, pa, pb, cs, cr, as_, ar, c2s, c2r, c3s, c3r, a2s, a2r, lsem,
):
    f = lax.axis_index("frame")
    h = lax.axis_index("height")
    d = lax.axis_index("dp")
    other = 1 - d
    me = h * ND + d
    barrier = pltpu.get_barrier_semaphore()
    for k in range(1, NF):
        pl.semaphore_signal(barrier, inc=1, **peer(frame=lax.rem(f + k, NF)))
    for k in range(1, NH * ND):
        q = lax.rem(me + k, NH * ND)
        pl.semaphore_signal(barrier, inc=1, **peer(height=q // ND, dp=lax.rem(q, ND)))
    pl.semaphore_wait(barrier, NF + NH * ND - 2)

    def remote(src, dst, ss, rs, **where):
        cp = pltpu.make_async_remote_copy(src_ref=src, dst_ref=dst, send_sem=ss, recv_sem=rs, **peer(**where))
        cp.start()
        return cp

    ca = remote(conv_ref.at[:, other], conv_a, pa.at[0], pb.at[0], dp=other)
    aa = remote(attn_ref.at[:, other], attn_a, pa.at[1], pb.at[1], dp=other)
    gic = []
    for k in range(1, NF):
        p = lax.rem(f + k, NF)
        gic.append(remote(gi_ref.at[pl.ds(2 * p, 2)], out_ref.at[:, f], gs.at[k], gr.at[k], frame=p))
    own = pltpu.make_async_copy(gi_ref.at[pl.ds(2 * f, 2)], out_ref.at[:, f], lsem.at[0])
    own.start()

    ca.wait_recv()
    for j in range(NH):
        conv_1[j] = (conv_ref[j, d].astype(F32) + conv_a[j].astype(F32)).astype(BF16)
    cc = []
    for k in range(1, NH):
        p = lax.rem(h + k, NH)
        cc.append(remote(conv_1.at[p], conv_b.at[k], cs.at[k], cr.at[k], height=p))
    aa.wait_recv()
    for j in range(NF):
        attn_1[j] = (attn_ref[j, d].astype(F32) + attn_a[j].astype(F32)).astype(BF16)
    ac = []
    for k in range(1, NF):
        p = lax.rem(f + k, NF)
        ac.append(remote(attn_1.at[p], attn_b.at[k], as_.at[k], ar.at[k], frame=p))

    total = attn_1[f].astype(F32)
    for k in range(1, NF):
        ac[k - 1].wait_recv()
        total = total + attn_b[k].astype(F32)
    for j in range(8):
        attn_c[j] = total[5 * j : 5 * j + 5, :]
    half = h // 4
    a2 = []
    for j in range(8):
        th, td = 4 * d + j // 2, j % 2
        mine = jnp.logical_and(th == h, td == d)

        @pl.when(jnp.logical_not(mine))
        def _(j=j, th=th, td=td):
            remote(attn_c.at[j], attn_cr.at[h], a2s.at[j], a2r.at[h], height=th, dp=td)

        @pl.when(mine)
        def _(j=j):
            attn_cr[h] = attn_c[j]

    total = conv_1[h].astype(F32)
    for k in range(1, NH):
        cc[k - 1].wait_recv()
        total = total + conv_b[k].astype(F32)
    conv_f[0:180, :] = total
    conv_f[180:192, :] = jnp.zeros((12, C), F32)
    for j in range(NF):
        conv_c[j] = conv_f[12 * j : 12 * j + 12, :].astype(BF16)
    c2 = []
    for k in range(1, NF):
        p = lax.rem(f + k, NF)
        c2.append(remote(conv_c.at[p], conv_cr.at[k], c2s.at[k], c2r.at[k], frame=p))
    total = conv_c[f].astype(F32)
    for k in range(1, NF):
        c2[k - 1].wait_recv()
        total = total + conv_cr[k].astype(F32)
    conv_d[...] = total.astype(BF16)
    c3 = []
    for k in range(1, NF):
        p = lax.rem(f + k, NF)
        c3.append(remote(conv_d, conv_dr.at[f], c3s.at[k], c3r.at[k], frame=p))
    conv_dr[f] = total.astype(BF16)

    def arrived(i):
        return pltpu.make_async_remote_copy(
            src_ref=attn_c.at[0], dst_ref=attn_cr.at[i], send_sem=a2s.at[i], recv_sem=a2r.at[i], **peer(dp=other)
        )

    for i in range(8):
        @pl.when(jnp.logical_not(jnp.logical_and(i == h, d == half)))
        def _(i=i):
            arrived(i).wait_recv()

    total = attn_cr[0]
    for i in range(1, 8):
        total = total + attn_cr[i]
    oattn_ref[...] = total

    for cp in c3:
        cp.wait_recv()
    for j in range(NF - 1):
        oconv_ref[12 * j : 12 * j + 12, :] = conv_dr[j].astype(F32)
    own.wait()
    for cp in gic:
        cp.wait_recv()
    for cp in [ca, aa] + gic + cc + ac + c2 + c3:
        cp.wait_send()
    for j in range(8):
        th, td = 4 * d + j // 2, j % 2

        @pl.when(jnp.logical_not(jnp.logical_and(th == h, td == d)))
        def _(j=j):
            arrived(j).wait_send()


def scatter_results(gi, attn, conv):
    vm = pl.BlockSpec(memory_space=pltpu.VMEM)
    v = pltpu.VMEM
    dma = pltpu.SemaphoreType.DMA
    return pl.pallas_call(
        scatter_kernel,
        out_shape=(
            jax.ShapeDtypeStruct((2, W, W, C), BF16),
            jax.ShapeDtypeStruct((5, C), F32),
            jax.ShapeDtypeStruct((180, C), F32),
        ),
        in_specs=[vm] * 3,
        out_specs=(vm, vm, vm),
        scratch_shapes=[
            v((NH, 180, C), BF16), v((NF, 40, C), BF16), v((NH, 180, C), BF16), v((NF, 40, C), BF16),
            v((NH, 180, C), BF16), v((NF, 40, C), BF16), v((192, C), F32), v((NF, 12, C), BF16), v((NF, 12, C), BF16),
            v((12, C), BF16), v((NF, 12, C), BF16), v((8, 5, C), F32), v((8, 5, C), F32),
            dma((NF,)), dma((NF,)), dma((2,)), dma((2,)), dma((NH,)), dma((NH,)), dma((NF,)), dma((NF,)),
            dma((NF,)), dma((NF,)), dma((NF,)), dma((NF,)), dma((8,)), dma((8,)), dma((1,)),
        ],
        compiler_params=pltpu.CompilerParams(collective_id=1, has_side_effects=True),
        name="scatter_results",
    )(gi, attn, conv)


def body(clip_latents, out_grad, box_mask, attn_weights, conv_weights, time_bias):
    x = clip_latents[0]
    dy = out_grad[0]
    marks = box_mask[0][..., None].astype(BF16)
    x_aug = jnp.concatenate([x, marks, jnp.zeros(x.shape[:3] + (CP - C - 1,), BF16)], axis=-1)
    xt, dy0, dyu, dyd = gather_rows(x_aug, dy)
    gi, attn, conv = compute(xt, dy0, dyu, dyd, attn_weights, conv_weights, time_bias)
    out, oattn, oconv = scatter_results(gi, attn, conv)
    return out[None], oattn, oconv


def solution(mesh):
    in_specs = (
        P("dp", "frame", "height", None, None),
        P("dp", "frame", "height", None, None),
        P("dp", "frame", "height", None),
        P(),
        P(),
        P(),
    )
    out_specs = (
        P("dp", "frame", "height", None, None),
        P(("frame", "height", "dp"), None),
        P(("height", "dp"), None),
    )
    return jax.shard_map(body, mesh=mesh, in_specs=in_specs, out_specs=out_specs, check_vma=False)
```

```python
import jax
import jax.numpy as jnp
from jax import lax
from jax.experimental import pallas as pl
from jax.experimental.pallas import tpu as pltpu
from jax.sharding import PartitionSpec as P

F32 = jnp.float32
BF16 = jnp.bfloat16
GROUND_BIAS = 2.0
NF, NH, ND = 16, 8, 2
C = 320
CP = 384
HEADS = 5
T = 32
W = 16
ROWS = T * W
BLK = 128
NB = ROWS // BLK
NEG = -1e30
TOKENS = 2 * 32 * 128 * 16
GRAD_SCALE = float(TOKENS) ** -0.5
SCALING = 0.125


def peer(**where):
    return dict(device_id=where, device_id_type=pl.DeviceIdType.MESH)


def nn(a, b):
    return lax.dot_general(a, b, (((1,), (0,)), ((), ())), preferred_element_type=F32)


def nt(a, b):
    return lax.dot_general(a, b, (((1,), (1,)), ((), ())), preferred_element_type=F32)


def tn(a, b):
    return lax.dot_general(a, b, (((0,), (0,)), ((), ())), preferred_element_type=F32)


def pixel_major(src, tr, store, width):
    for s in range(0, width, 128):
        w = min(128, width - s)
        tr[s // 128, :, :w] = src[:, :, s : s + w].reshape(ROWS, w).astype(F32)
    for p in range(W):
        for s in range(0, width, 128):
            w = min(128, width - s)
            store(p, s, w, tr[s // 128, pl.ds(p, T, stride=W), :][:, :w].astype(BF16))


SLABS = ((0, 128, (0, 1)), (128, 128, (2, 3)), (256, 64, (4,)))


def block_kernel(
    x_ref, dy_ref, mark_ref, wat_ref, wct_ref, tb_ref,
    out_ref, attn_cr, conv_dr,
    xs, xt, dy0, dyu, dyd, wa, wc,
    tr, xp, dyp, q_s, k_s, v_s, o_s, pr, bias_s, y1_s, a_t, da_s, g_s, do_s, dq_s, dk_s, dv_s, x_t, o_t, cf,
    gi_s, attn_l, conv_l, conv_a, attn_a, conv_1, attn_1, conv_b, attn_b, conv_f, conv_c, conv_cr, conv_d, attn_c,
    xss, xsr, dss, dsr, hs, hr, gs, gr, pa, pb, cs, cr, as_, ar, c2s, c2r, c3s, c3r, a2s, a2r, lsem,
):
    f = lax.axis_index("frame")
    h = lax.axis_index("height")
    d = lax.axis_index("dp")
    other = 1 - d
    me = h * ND + d
    lin = h * NF + f
    prev = lax.rem(lin + NF * NH - 1, NF * NH)
    nxt = lax.rem(lin + 1, NF * NH)

    def remote(src, dst, ss, rs, **where):
        cp = pltpu.make_async_remote_copy(src_ref=src, dst_ref=dst, send_sem=ss, recv_sem=rs, **peer(**where))
        cp.start()
        return cp

    barrier = pltpu.get_barrier_semaphore()
    for k in range(1, NF):
        pl.semaphore_signal(barrier, inc=1, **peer(frame=lax.rem(f + k, NF)))
    for k in range(1, NH * ND):
        q = lax.rem(me + k, NH * ND)
        pl.semaphore_signal(barrier, inc=1, **peer(height=q // ND, dp=lax.rem(q, ND)))

    @pl.when(f == 0)
    def _():
        pl.semaphore_signal(barrier, inc=1, **peer(frame=lax.rem(prev, NF), height=prev // NF))

    @pl.when(f == NF - 1)
    def _():
        pl.semaphore_signal(barrier, inc=1, **peer(frame=lax.rem(nxt, NF), height=nxt // NF))

    lwa = pltpu.make_async_copy(wat_ref, wa, lsem.at[0])
    lwc = pltpu.make_async_copy(wct_ref, wc, lsem.at[1])
    lwa.start()
    lwc.start()

    xs[:, :, :, 0:256] = x_ref[:, :, :, 0:256]
    eye = lax.broadcasted_iota(jnp.int32, (1, W, W), 1) == lax.broadcasted_iota(jnp.int32, (1, W, W), 2)
    lane3 = lax.broadcasted_iota(jnp.int32, (1, W, 128), 2)
    for fr in range(2):
        mk = mark_ref[fr].astype(F32)
        col = jnp.sum(jnp.where(eye, mk[:, None, :], 0.0), axis=-1, keepdims=True)
        xs[fr, :, :, 256:384] = jnp.where(lane3 == 64, col, 0.0).astype(BF16)
    xs[:, :, :, 256:320] = x_ref[:, :, :, 256:320]

    edge = jnp.where(jnp.logical_or(f == 0, f == NF - 1), 1, 0)
    pl.semaphore_wait(barrier, NF + NH * ND - 2 + edge)

    xc, dc = [], []
    for k in range(1, NF):
        p = lax.rem(f + k, NF)
        xc.append(remote(xs.at[:, p], xt.at[pl.ds(2 * f, 2)], xss.at[k], xsr.at[k], frame=p))
    for k in range(1, NF):
        p = lax.rem(f + k, NF)
        dc.append(remote(dy_ref.at[:, p], dy0.at[pl.ds(2 * f, 2)], dss.at[k], dsr.at[k], frame=p))
    lx = pltpu.make_async_copy(xs.at[:, f], xt.at[pl.ds(2 * f, 2)], lsem.at[2])
    ld = pltpu.make_async_copy(dy_ref.at[:, f], dy0.at[pl.ds(2 * f, 2)], lsem.at[3])
    lx.start()
    ld.start()

    ri = lax.broadcasted_iota(jnp.int32, (BLK, BLK), 0) // T
    ci = lax.broadcasted_iota(jnp.int32, (BLK, BLK), 1) // T
    for hd in range(HEADS):
        one = tb_ref[hd]
        wide = jnp.concatenate([one] * 4, axis=1)
        full = jnp.concatenate([wide] * 4, axis=0)
        bias_s[hd] = jnp.where(ri == ci, full, NEG)
    zero = jnp.zeros((T, C), BF16)
    for r in range(3):
        dyp[r, 0:T, :] = zero
        dyp[r, (W + 1) * T :, :] = zero
    lane = lax.broadcasted_iota(jnp.int32, (BLK, 128), 1)
    low = lane < 64
    ones = jnp.full((8, 128), GROUND_BIAS, BF16)

    def only(val, i, w):
        if w == 64:
            return val
        keep = low if i == 0 else jnp.logical_not(low)
        return jnp.where(keep, val, jnp.zeros_like(val))

    def pick(parts, w):
        if w == 64:
            return parts[0]
        return jnp.where(low, parts[0], parts[1])

    lwa.wait()
    lx.wait()
    for cp in xc:
        cp.wait_recv()

    def put_x(p, s, w, val):
        xp[p * T : (p + 1) * T, s : s + w] = val

    pixel_major(xt, tr, put_x, CP)
    x = xp[:, :C]
    q_s[...] = nt(x, wa[:, 0:C]).astype(BF16)
    k_s[...] = nt(x, wa[:, C : 2 * C]).astype(BF16)
    v_s[...] = nt(x, wa[:, 2 * C : 3 * C]).astype(BF16)

    for b in range(NB):
        rows = slice(b * BLK, (b + 1) * BLK)
        marks = jnp.where(lane == 64, xp[rows, 256:384], jnp.zeros((BLK, 128), BF16))
        key_bias = nt(ones, marks)[0:1, :]
        for s, w, heads in SLABS:
            ls = slice(s, s + w)
            qb, kb, vb = q_s[rows, ls], k_s[rows, ls], v_s[rows, ls]
            outs = []
            for i, hd in enumerate(heads):
                sc = nt(only(qb, i, w), kb) * SCALING + bias_s[hd] + key_bias
                e = jnp.exp(sc - jnp.max(sc, axis=-1, keepdims=True))
                pf = e / jnp.sum(e, axis=-1, keepdims=True)
                pr[b, hd] = pf
                outs.append(nn(pf.astype(BF16), vb))
            o_s[rows, ls] = pick(outs, w).astype(BF16)

    ld.wait()
    for cp in dc:
        cp.wait_recv()
    up = remote(dy0, dyd, hs.at[0], hr.at[0], frame=lax.rem(prev, NF), height=prev // NF)
    down = remote(dy0, dyu, hs.at[1], hr.at[1], frame=lax.rem(nxt, NF), height=nxt // NF)

    y1 = (x.astype(F32) + nt(o_s[...], wa[:, 3 * C :])).astype(BF16)
    y1_s[...] = y1
    yf = y1.astype(F32)
    act = yf / (1.0 + jnp.exp(-yf))
    a_t[...] = act.T.astype(BF16)

    def place_row(r, src, keep):
        def put(p, s, w, val):
            if keep is not None:
                val = jnp.where(keep, val, jnp.zeros_like(val))
            dyp[r, (p + 1) * T : (p + 2) * T, s : s + w] = val

        pixel_major(src, tr, put, C)

    def tap_row(r, first):
        for c in range(3):
            tap = 3 * r + c
            off = (2 - c) * T
            shifted = dyp[r, off : off + ROWS, :]
            part = nn(shifted, wc[:, tap * C : (tap + 1) * C])
            da_s[...] = part if first else da_s[...] + part
            first = False
            cf[tap * C : (tap + 1) * C, :] = nn(a_t[...], shifted) * GRAD_SCALE

    lwc.wait()
    place_row(1, dy0, None)
    tap_row(1, True)
    x_t[...] = x.astype(F32).T.astype(BF16)
    o_t[...] = o_s[...].astype(F32).T.astype(BF16)
    up.wait_recv()
    place_row(0, dyd, lin < NF * NH - 1)
    tap_row(0, False)
    down.wait_recv()
    place_row(2, dyu, lin > 0)
    tap_row(2, False)

    for k in range(NH * ND):
        conv_l[k // ND, k % ND] = cf[k * 180 : (k + 1) * 180, :].astype(BF16)
    ca = remote(conv_l.at[:, other], conv_a, pa.at[0], pb.at[0], dp=other)

    yf = y1_s[...].astype(F32)
    sig = 1.0 / (1.0 + jnp.exp(-yf))
    slope = sig * (1.0 + yf * (1.0 - sig))
    g = (dyp[1, T : T + ROWS, :].astype(F32) + slope * da_s[...]).astype(BF16)
    g_s[...] = g
    do_s[...] = nn(g, wa[:, 3 * C :]).astype(BF16)

    ca.wait_recv()
    for j in range(NH):
        conv_1[j] = (conv_l[j, d].astype(F32) + conv_a[j].astype(F32)).astype(BF16)
    cc = []
    for k in range(1, NH):
        p = lax.rem(h + k, NH)
        cc.append(remote(conv_1.at[p], conv_b.at[k], cs.at[k], cr.at[k], height=p))

    for b in range(NB):
        rows = slice(b * BLK, (b + 1) * BLK)
        for s, w, heads in SLABS:
            ls = slice(s, s + w)
            qb, kb, vb, db = q_s[rows, ls], k_s[rows, ls], v_s[rows, ls], do_s[rows, ls]
            dqs, dks, dvs = [], [], []
            for i, hd in enumerate(heads):
                pf = pr[b, hd]
                dp = nt(only(db, i, w), vb)
                dsc = (pf * (dp - jnp.sum(pf * dp, axis=-1, keepdims=True))).astype(BF16)
                dqs.append(nn(dsc, kb))
                dks.append(tn(dsc, qb))
                dvs.append(tn(pf.astype(BF16), db))
            dq_s[rows, ls] = (pick(dqs, w) * SCALING).astype(BF16)
            dk_s[rows, ls] = (pick(dks, w) * SCALING).astype(BF16)
            dv_s[rows, ls] = pick(dvs, w).astype(BF16)

    dx = nn(dq_s[...], wa[:, 0:C]) + nn(dk_s[...], wa[:, C : 2 * C]) + nn(dv_s[...], wa[:, 2 * C : 3 * C])
    gi = g_s[...].astype(F32) + dx.astype(BF16).astype(F32)
    for s in range(0, C, 128):
        w = min(128, C - s)
        tr[s // 128, :, :w] = gi[:, s : s + w]
    for t in range(T):
        for s in range(0, C, 128):
            w = min(128, C - s)
            gi_s[t, :, s : s + w] = tr[s // 128, pl.ds(t, W, stride=T), :][:, :w].astype(BF16)
    gic = []
    for k in range(1, NF):
        p = lax.rem(f + k, NF)
        gic.append(remote(gi_s.at[pl.ds(2 * p, 2)], out_ref.at[:, f], gs.at[k], gr.at[k], frame=p))
    own = pltpu.make_async_copy(gi_s.at[pl.ds(2 * f, 2)], out_ref.at[:, f], lsem.at[4])
    own.start()

    for j, (left, right) in enumerate(((x_t, dq_s), (x_t, dk_s), (x_t, dv_s), (o_t, g_s))):
        term = nn(left[...], right[...]) * GRAD_SCALE
        for k in range(8):
            m = 8 * j + k
            attn_l[m // 2, m % 2] = term[40 * k : 40 * (k + 1), :].astype(BF16)
    aa = remote(attn_l.at[:, other], attn_a, pa.at[1], pb.at[1], dp=other)
    aa.wait_recv()
    for j in range(NF):
        attn_1[j] = (attn_l[j, d].astype(F32) + attn_a[j].astype(F32)).astype(BF16)
    ac = []
    for k in range(1, NF):
        p = lax.rem(f + k, NF)
        ac.append(remote(attn_1.at[p], attn_b.at[k], as_.at[k], ar.at[k], frame=p))

    total = conv_1[h].astype(F32)
    for k in range(1, NH):
        cc[k - 1].wait_recv()
        total = total + conv_b[k].astype(F32)
    conv_f[0:180, :] = total
    conv_f[180:192, :] = jnp.zeros((12, C), F32)
    for j in range(NF):
        conv_c[j] = conv_f[12 * j : 12 * j + 12, :].astype(BF16)
    c2 = []
    for k in range(1, NF):
        p = lax.rem(f + k, NF)
        c2.append(remote(conv_c.at[p], conv_cr.at[k], c2s.at[k], c2r.at[k], frame=p))

    total = attn_1[f].astype(F32)
    for k in range(1, NF):
        ac[k - 1].wait_recv()
        total = total + attn_b[k].astype(F32)
    for j in range(8):
        attn_c[j] = total[5 * j : 5 * j + 5, :]
    half = h // 4
    for j in range(8):
        th, td = 4 * d + j // 2, j % 2
        mine = jnp.logical_and(th == h, td == d)

        @pl.when(jnp.logical_not(mine))
        def _(j=j, th=th, td=td):
            remote(attn_c.at[j], attn_cr.at[h], a2s.at[j], a2r.at[h], height=th, dp=td)

        @pl.when(mine)
        def _(j=j):
            attn_cr[h] = attn_c[j]

    total = conv_c[f].astype(F32)
    for k in range(1, NF):
        c2[k - 1].wait_recv()
        total = total + conv_cr[k].astype(F32)
    conv_d[...] = total.astype(BF16)
    c3 = []
    for k in range(1, NF):
        p = lax.rem(f + k, NF)
        c3.append(remote(conv_d, conv_dr.at[f], c3s.at[k], c3r.at[k], frame=p))
    conv_dr[f] = total.astype(BF16)

    def arrived(i):
        return pltpu.make_async_remote_copy(
            src_ref=attn_c.at[0], dst_ref=attn_cr.at[i], send_sem=a2s.at[i], recv_sem=a2r.at[i], **peer(dp=other)
        )

    for i in range(8):
        @pl.when(jnp.logical_not(jnp.logical_and(i == h, d == half)))
        def _(i=i):
            arrived(i).wait_recv()

    own.wait()
    for cp in c3 + gic:
        cp.wait_recv()
    for cp in xc + dc + [up, down, ca, aa] + gic + cc + ac + c2 + c3:
        cp.wait_send()
    for j in range(8):
        th, td = 4 * d + j // 2, j % 2

        @pl.when(jnp.logical_not(jnp.logical_and(th == h, td == d)))
        def _(j=j):
            arrived(j).wait_send()


def block(x, dy, marks, wat, wct, tb):
    vm = pl.BlockSpec(memory_space=pltpu.VMEM)
    anyw = pl.BlockSpec(memory_space=pl.ANY)
    v = pltpu.VMEM
    dma = pltpu.SemaphoreType.DMA
    tok = v((ROWS, C), BF16)
    row = v((T, W, C), BF16)
    return pl.pallas_call(
        block_kernel,
        out_shape=(
            jax.ShapeDtypeStruct((2, W, W, C), BF16),
            jax.ShapeDtypeStruct((8, 5, C), F32),
            jax.ShapeDtypeStruct((NF, 12, C), BF16),
        ),
        in_specs=[vm, vm, vm, anyw, anyw, vm],
        out_specs=(vm, vm, vm),
        scratch_shapes=[
            v((2, W, W, CP), BF16), v((T, W, CP), BF16), row, row, row, v((C, 4 * C), BF16), v((C, 9 * C), BF16),
            v((3, ROWS, 128), F32), v((ROWS, CP), BF16), v((3, ROWS + 2 * T, C), BF16),
            tok, tok, tok, tok,
            v((NB, HEADS, BLK, BLK), F32), v((HEADS, BLK, BLK), F32),
            tok, v((C, ROWS), BF16), v((ROWS, C), F32), tok, tok, tok, tok, tok,
            v((C, ROWS), BF16), v((C, ROWS), BF16), v((9 * C, C), F32),
            row, v((NF, ND, 40, C), BF16), v((NH, ND, 180, C), BF16),
            v((NH, 180, C), BF16), v((NF, 40, C), BF16), v((NH, 180, C), BF16), v((NF, 40, C), BF16),
            v((NH, 180, C), BF16), v((NF, 40, C), BF16), v((192, C), F32), v((NF, 12, C), BF16), v((NF, 12, C), BF16),
            v((12, C), BF16), v((8, 5, C), F32),
            dma((NF,)), dma((NF,)), dma((NF,)), dma((NF,)), dma((2,)), dma((2,)),
            dma((NF,)), dma((NF,)), dma((2,)), dma((2,)), dma((NH,)), dma((NH,)), dma((NF,)), dma((NF,)),
            dma((NF,)), dma((NF,)), dma((NF,)), dma((NF,)), dma((8,)), dma((8,)), dma((5,)),
        ],
        compiler_params=pltpu.CompilerParams(collective_id=0, has_side_effects=True),
        name="block_backward",
    )(x, dy, marks, wat, wct, tb)


def finish_kernel(gi_ref, attn_ref, conv_ref, out_ref, oattn_ref, oconv_ref):
    out_ref[...] = gi_ref[...]
    total = attn_ref[0]
    for i in range(1, 8):
        total = total + attn_ref[i]
    oattn_ref[...] = total
    for j in range(NF - 1):
        oconv_ref[12 * j : 12 * j + 12, :] = conv_ref[j].astype(F32)


def finish(gi, attn, conv):
    vm = pl.BlockSpec(memory_space=pltpu.VMEM)
    return pl.pallas_call(
        finish_kernel,
        out_shape=(
            jax.ShapeDtypeStruct((2, W, W, C), BF16),
            jax.ShapeDtypeStruct((5, C), F32),
            jax.ShapeDtypeStruct((180, C), F32),
        ),
        in_specs=[vm] * 3,
        out_specs=(vm, vm, vm),
        name="finish",
    )(gi, attn, conv)


def body(clip_latents, out_grad, box_mask, attn_weights, conv_weights, time_bias):
    got = block(clip_latents[0], out_grad[0], box_mask[0], attn_weights.T, conv_weights.T, time_bias)
    out, oattn, oconv = finish(*got)
    return out[None], oattn, oconv


def solution(mesh):
    in_specs = (
        P("dp", "frame", "height", None, None),
        P("dp", "frame", "height", None, None),
        P("dp", "frame", "height", None),
        P(),
        P(),
        P(),
    )
    out_specs = (
        P("dp", "frame", "height", None, None),
        P(("frame", "height", "dp"), None),
        P(("height", "dp"), None),
    )
    return jax.shard_map(body, mesh=mesh, in_specs=in_specs, out_specs=out_specs, check_vma=False)
```

```python
import jax
import jax.numpy as jnp
from jax import lax
from jax.experimental import pallas as pl
from jax.experimental.pallas import tpu as pltpu
from jax.sharding import PartitionSpec as P

F32 = jnp.float32
BF16 = jnp.bfloat16
GROUND_BIAS = 2.0
NF, NH, ND = 16, 8, 2
C = 320
CP = 384
HEADS = 5
T = 32
W = 16
ROWS = T * W
BLK = 128
NB = ROWS // BLK
NEG = -1e30
TOKENS = 2 * 32 * 128 * 16
GRAD_SCALE = float(TOKENS) ** -0.5
SCALING = 0.125


def peer(**where):
    return dict(device_id=where, device_id_type=pl.DeviceIdType.MESH)


def nn(a, b):
    return lax.dot_general(a, b, (((1,), (0,)), ((), ())), preferred_element_type=F32)


def nt(a, b):
    return lax.dot_general(a, b, (((1,), (1,)), ((), ())), preferred_element_type=F32)


def tn(a, b):
    return lax.dot_general(a, b, (((0,), (0,)), ((), ())), preferred_element_type=F32)


def pixel_major(src, tr, store, width):
    for s in range(0, width, 128):
        w = min(128, width - s)
        tr[s // 128, :, :w] = src[:, :, s : s + w].reshape(ROWS, w).astype(F32)
    for p in range(W):
        for s in range(0, width, 128):
            w = min(128, width - s)
            store(p, s, w, tr[s // 128, pl.ds(p, T, stride=W), :][:, :w].astype(BF16))


ORDER = (1, 15, 8, 2, 14, 7, 9, 3, 13, 6, 10, 4, 12, 5, 11)
SLABS = ((0, 128, (0, 1)), (128, 128, (2, 3)), (256, 64, (4,)))


def block_kernel(
    x_ref, dy_ref, mark_ref, wat_ref, wct_ref, tb_ref,
    out_ref, attn_cr, conv_dr,
    xs, xt, dy0, dyu, dyd, wa, wc,
    tr, xp, dyp, q_s, k_s, v_s, o_s, pr, bias_s, y1_s, a_t, da_s, g_s, do_s, dq_s, dk_s, dv_s, x_t, o_t, cf,
    gi_s, attn_f, attn_l, conv_l, conv_a, attn_a, conv_1, attn_1, conv_b, attn_b, conv_f, conv_c, conv_cr, conv_d, attn_g, attn_c,
    xss, xsr, dss, dsr, hs, hr, gs, gr, pa, pb, cs, cr, as_, ar, c2s, c2r, c3s, c3r, a2s, a2r, lsem,
):
    f = lax.axis_index("frame")
    h = lax.axis_index("height")
    d = lax.axis_index("dp")
    other = 1 - d
    me = h * ND + d
    lin = h * NF + f
    prev = lax.rem(lin + NF * NH - 1, NF * NH)
    nxt = lax.rem(lin + 1, NF * NH)

    def remote(src, dst, ss, rs, **where):
        cp = pltpu.make_async_remote_copy(src_ref=src, dst_ref=dst, send_sem=ss, recv_sem=rs, **peer(**where))
        cp.start()
        return cp

    barrier = pltpu.get_barrier_semaphore()
    for k in range(1, NF):
        pl.semaphore_signal(barrier, inc=1, **peer(frame=lax.rem(f + k, NF)))
    for k in range(1, NH * ND):
        q = lax.rem(me + k, NH * ND)
        pl.semaphore_signal(barrier, inc=1, **peer(height=q // ND, dp=lax.rem(q, ND)))

    @pl.when(f == 0)
    def _():
        pl.semaphore_signal(barrier, inc=1, **peer(frame=lax.rem(prev, NF), height=prev // NF))

    @pl.when(f == NF - 1)
    def _():
        pl.semaphore_signal(barrier, inc=1, **peer(frame=lax.rem(nxt, NF), height=nxt // NF))

    lwa = pltpu.make_async_copy(wat_ref, wa, lsem.at[0])
    lwc = pltpu.make_async_copy(wct_ref, wc, lsem.at[1])
    lwa.start()
    lwc.start()

    xs[:, :, :, 0:256] = x_ref[:, :, :, 0:256]
    eye = lax.broadcasted_iota(jnp.int32, (1, W, W), 1) == lax.broadcasted_iota(jnp.int32, (1, W, W), 2)
    lane3 = lax.broadcasted_iota(jnp.int32, (1, W, 128), 2)
    for fr in range(2):
        mk = mark_ref[fr].astype(F32)
        col = jnp.sum(jnp.where(eye, mk[:, None, :], 0.0), axis=-1, keepdims=True)
        xs[fr, :, :, 256:384] = jnp.where(lane3 == 64, col, 0.0).astype(BF16)
    xs[:, :, :, 256:320] = x_ref[:, :, :, 256:320]

    edge = jnp.where(jnp.logical_or(f == 0, f == NF - 1), 1, 0)
    pl.semaphore_wait(barrier, NF + NH * ND - 2 + edge)

    xc, dc = [], []
    for k in range(1, NF):
        p = lax.rem(f + k, NF)
        xc.append(remote(xs.at[:, p], xt.at[pl.ds(2 * f, 2)], xss.at[k], xsr.at[k], frame=p))
    for k in range(1, NF):
        p = lax.rem(f + k, NF)
        dc.append(remote(dy_ref.at[:, p], dy0.at[pl.ds(2 * f, 2)], dss.at[k], dsr.at[k], frame=p))
    lx = pltpu.make_async_copy(xs.at[:, f], xt.at[pl.ds(2 * f, 2)], lsem.at[2])
    ld = pltpu.make_async_copy(dy_ref.at[:, f], dy0.at[pl.ds(2 * f, 2)], lsem.at[3])
    lx.start()
    ld.start()
    fwd = []

    def forward(k):
        part = pl.ds(2 * lax.rem(f + NF - k, NF), 2)
        up = remote(dy0.at[part], dyd.at[part], hs.at[0, k], hr.at[0, k], frame=lax.rem(prev, NF), height=prev // NF)
        down = remote(dy0.at[part], dyu.at[part], hs.at[1, k], hr.at[1, k], frame=lax.rem(nxt, NF), height=nxt // NF)
        fwd.append((up, down))

    ld.wait()
    forward(0)
    waiting = list(ORDER)

    def forward_next():
        if waiting:
            k = waiting.pop(0)
            dc[k - 1].wait_recv()
            forward(k)

    ri = lax.broadcasted_iota(jnp.int32, (BLK, BLK), 0) // T
    ci = lax.broadcasted_iota(jnp.int32, (BLK, BLK), 1) // T
    for hd in range(HEADS):
        one = tb_ref[hd]
        wide = jnp.concatenate([one] * 4, axis=1)
        full = jnp.concatenate([wide] * 4, axis=0)
        bias_s[hd] = jnp.where(ri == ci, full, NEG)
    zero = jnp.zeros((T, C), BF16)
    for r in range(3):
        dyp[r, 0:T, :] = zero
        dyp[r, (W + 1) * T :, :] = zero
    lane = lax.broadcasted_iota(jnp.int32, (BLK, 128), 1)
    low = lane < 64
    ones = jnp.full((8, 128), GROUND_BIAS, BF16)

    def only(val, i, w):
        if w == 64:
            return val
        keep = low if i == 0 else jnp.logical_not(low)
        return jnp.where(keep, val, jnp.zeros_like(val))

    def pick(parts, w):
        if w == 64:
            return parts[0]
        return jnp.where(low, parts[0], parts[1])

    lwa.wait()
    lx.wait()
    for k in ORDER:
        xc[k - 1].wait_recv()

    def put_x(p, s, w, val):
        xp[p * T : (p + 1) * T, s : s + w] = val

    pixel_major(xt, tr, put_x, CP)
    x = xp[:, :C]
    q_s[...] = nt(x, wa[:, 0:C]).astype(BF16)
    k_s[...] = nt(x, wa[:, C : 2 * C]).astype(BF16)
    v_s[...] = nt(x, wa[:, 2 * C : 3 * C]).astype(BF16)

    for b in range(NB):
        rows = slice(b * BLK, (b + 1) * BLK)
        marks = jnp.where(lane == 64, xp[rows, 256:384], jnp.zeros((BLK, 128), BF16))
        key_bias = nt(ones, marks)[0:1, :]
        for s, w, heads in SLABS:
            ls = slice(s, s + w)
            qb, kb, vb = q_s[rows, ls], k_s[rows, ls], v_s[rows, ls]
            outs = []
            for i, hd in enumerate(heads):
                sc = nt(only(qb, i, w), kb) * SCALING + bias_s[hd] + key_bias
                e = jnp.exp(sc - jnp.max(sc, axis=-1, keepdims=True))
                pf = e / jnp.sum(e, axis=-1, keepdims=True)
                pr[b, hd] = pf
                outs.append(nn(pf.astype(BF16), vb))
            o_s[rows, ls] = pick(outs, w).astype(BF16)
            forward_next()
    while waiting:
        forward_next()

    y1 = (x.astype(F32) + nt(o_s[...], wa[:, 3 * C :])).astype(BF16)
    y1_s[...] = y1
    yf = y1.astype(F32)
    act = yf / (1.0 + jnp.exp(-yf))
    a_t[...] = act.T.astype(BF16)

    def place_row(r, src, keep):
        def put(p, s, w, val):
            if keep is not None:
                val = jnp.where(keep, val, jnp.zeros_like(val))
            dyp[r, (p + 1) * T : (p + 2) * T, s : s + w] = val

        pixel_major(src, tr, put, C)

    def tap_row(r, first):
        for c in range(3):
            tap = 3 * r + c
            off = (2 - c) * T
            shifted = dyp[r, off : off + ROWS, :]
            part = nn(shifted, wc[:, tap * C : (tap + 1) * C])
            da_s[...] = part if first else da_s[...] + part
            first = False
            cf[tap * C : (tap + 1) * C, :] = nn(a_t[...], shifted) * GRAD_SCALE

    lwc.wait()
    place_row(1, dy0, None)
    tap_row(1, True)
    rr = lax.broadcasted_iota(jnp.int32, (C, C), 0)
    cc_ = lax.broadcasted_iota(jnp.int32, (C, C), 1)
    mm = (rr * 3277) >> 16
    rem = rr - 20 * mm
    cf_ = (rem * 13108) >> 16
    perm = jnp.where(cc_ == 80 * cf_ + 5 * mm + (rem - 5 * cf_), 1.0, 0.0).astype(BF16)
    x_t[...] = nt(perm, x).astype(BF16)
    o_t[...] = nt(perm, o_s[...]).astype(BF16)
    for up, _ in fwd:
        up.wait_recv()
    place_row(0, dyd, lin < NF * NH - 1)
    tap_row(0, False)
    for _, down in fwd:
        down.wait_recv()
    place_row(2, dyu, lin > 0)
    tap_row(2, False)

    for k in range(NH * ND):
        conv_l[k // ND, k % ND] = cf[k * 180 : (k + 1) * 180, :].astype(BF16)
    ca = remote(conv_l.at[:, other], conv_a, pa.at[0], pb.at[0], dp=other)

    yf = y1_s[...].astype(F32)
    sig = 1.0 / (1.0 + jnp.exp(-yf))
    slope = sig * (1.0 + yf * (1.0 - sig))
    g = (dyp[1, T : T + ROWS, :].astype(F32) + slope * da_s[...]).astype(BF16)
    g_s[...] = g
    do_s[...] = nn(g, wa[:, 3 * C :]).astype(BF16)

    ca.wait_recv()
    for j in range(NH):
        conv_1[j] = (conv_l[j, d].astype(F32) + conv_a[j].astype(F32)).astype(BF16)
    cc = []
    for k in range(1, NH):
        p = lax.rem(h + k, NH)
        cc.append(remote(conv_1.at[p], conv_b.at[k], cs.at[k], cr.at[k], height=p))

    for b in range(NB):
        rows = slice(b * BLK, (b + 1) * BLK)
        for s, w, heads in SLABS:
            ls = slice(s, s + w)
            qb, kb, vb, db = q_s[rows, ls], k_s[rows, ls], v_s[rows, ls], do_s[rows, ls]
            dqs, dks, dvs = [], [], []
            for i, hd in enumerate(heads):
                pf = pr[b, hd]
                dp = nt(only(db, i, w), vb)
                dsc = (pf * (dp - jnp.sum(pf * dp, axis=-1, keepdims=True))).astype(BF16)
                dqs.append(nn(dsc, kb))
                dks.append(tn(dsc, qb))
                dvs.append(tn(pf.astype(BF16), db))
            dq_s[rows, ls] = (pick(dqs, w) * SCALING).astype(BF16)
            dk_s[rows, ls] = (pick(dks, w) * SCALING).astype(BF16)
            dv_s[rows, ls] = pick(dvs, w).astype(BF16)

    dx = nn(dq_s[...], wa[:, 0:C]) + nn(dk_s[...], wa[:, C : 2 * C]) + nn(dv_s[...], wa[:, 2 * C : 3 * C])
    gi = g_s[...].astype(F32) + dx.astype(BF16).astype(F32)
    for s in range(0, C, 128):
        w = min(128, C - s)
        tr[s // 128, :, :w] = gi[:, s : s + w]
    for t in range(T):
        for s in range(0, C, 128):
            w = min(128, C - s)
            gi_s[t, :, s : s + w] = tr[s // 128, pl.ds(t, W, stride=T), :][:, :w].astype(BF16)
    gic = []
    for k in range(1, NF):
        p = lax.rem(f + k, NF)
        gic.append(remote(gi_s.at[pl.ds(2 * p, 2)], out_ref.at[:, f], gs.at[k], gr.at[k], frame=p))
    own = pltpu.make_async_copy(gi_s.at[pl.ds(2 * f, 2)], out_ref.at[:, f], lsem.at[4])
    own.start()

    for j, (left, right) in enumerate(((x_t, dq_s), (x_t, dk_s), (x_t, dv_s), (o_t, g_s))):
        term = nn(left[...], right[...]) * GRAD_SCALE
        for m in range(NH * ND):
            attn_f[m, 20 * j : 20 * j + 20, :] = term[20 * m : 20 * m + 20, :]
    for m in range(NH * ND):
        attn_l[m // ND, m % ND] = attn_f[m].astype(BF16)
    aa = remote(attn_l.at[:, other], attn_a, pa.at[1], pb.at[1], dp=other)
    aa.wait_recv()
    for j in range(NH):
        attn_1[j] = (attn_l[j, d].astype(F32) + attn_a[j].astype(F32)).astype(BF16)
    ac = []
    for k in range(1, NH):
        p = lax.rem(h + k, NH)
        ac.append(remote(attn_1.at[p], attn_b.at[k], as_.at[k], ar.at[k], height=p))

    total = conv_1[h].astype(F32)
    for k in range(1, NH):
        cc[k - 1].wait_recv()
        total = total + conv_b[k].astype(F32)
    conv_f[0:180, :] = total
    conv_f[180:192, :] = jnp.zeros((12, C), F32)
    for j in range(NF):
        conv_c[j] = conv_f[12 * j : 12 * j + 12, :].astype(BF16)
    c2 = []
    for k in range(1, NF):
        p = lax.rem(f + k, NF)
        c2.append(remote(conv_c.at[p], conv_cr.at[k], c2s.at[k], c2r.at[k], frame=p))

    total = attn_1[h].astype(F32)
    for k in range(1, NH):
        ac[k - 1].wait_recv()
        total = total + attn_b[k].astype(F32)
    attn_g[...] = total
    for j in range(NF):
        attn_c[j] = attn_g[5 * j : 5 * j + 5, :]
    a2 = []
    for k in range(1, NF):
        p = lax.rem(f + k, NF)
        a2.append(remote(attn_c.at[p], attn_cr.at[k], a2s.at[k], a2r.at[k], frame=p))
    attn_cr[0] = attn_c[f]

    total = conv_c[f].astype(F32)
    for k in range(1, NF):
        c2[k - 1].wait_recv()
        total = total + conv_cr[k].astype(F32)
    conv_d[...] = total.astype(BF16)
    c3 = []
    for k in range(1, NF):
        p = lax.rem(f + k, NF)
        c3.append(remote(conv_d, conv_dr.at[f], c3s.at[k], c3r.at[k], frame=p))
    conv_dr[f] = total.astype(BF16)

    own.wait()
    for cp in a2 + c3 + gic:
        cp.wait_recv()
    for cp in xc + dc + [ca, aa] + gic + cc + ac + a2 + c2 + c3:
        cp.wait_send()
    for up, down in fwd:
        up.wait_send()
        down.wait_send()


def block(x, dy, marks, wat, wct, tb):
    vm = pl.BlockSpec(memory_space=pltpu.VMEM)
    anyw = pl.BlockSpec(memory_space=pl.ANY)
    v = pltpu.VMEM
    dma = pltpu.SemaphoreType.DMA
    tok = v((ROWS, C), BF16)
    row = v((T, W, C), BF16)
    return pl.pallas_call(
        block_kernel,
        out_shape=(
            jax.ShapeDtypeStruct((2, W, W, C), BF16),
            jax.ShapeDtypeStruct((NF, 5, C), F32),
            jax.ShapeDtypeStruct((NF, 12, C), BF16),
        ),
        in_specs=[vm, vm, vm, anyw, anyw, vm],
        out_specs=(vm, vm, vm),
        scratch_shapes=[
            v((2, W, W, CP), BF16), v((T, W, CP), BF16), row, row, row, v((C, 4 * C), BF16), v((C, 9 * C), BF16),
            v((3, ROWS, 128), F32), v((ROWS, CP), BF16), v((3, ROWS + 2 * T, C), BF16),
            tok, tok, tok, tok,
            v((NB, HEADS, BLK, BLK), F32), v((HEADS, BLK, BLK), F32),
            tok, v((C, ROWS), BF16), v((ROWS, C), F32), tok, tok, tok, tok, tok,
            v((C, ROWS), BF16), v((C, ROWS), BF16), v((9 * C, C), F32),
            row, v((NH * ND, 80, C), F32), v((NH, ND, 80, C), BF16), v((NH, ND, 180, C), BF16),
            v((NH, 180, C), BF16), v((NH, 80, C), BF16), v((NH, 180, C), BF16), v((NH, 80, C), BF16),
            v((NH, 180, C), BF16), v((NH, 80, C), BF16), v((192, C), F32), v((NF, 12, C), BF16), v((NF, 12, C), BF16),
            v((12, C), BF16), v((80, C), F32), v((NF, 5, C), F32),
            dma((NF,)), dma((NF,)), dma((NF,)), dma((NF,)), dma((2, NF)), dma((2, NF)),
            dma((NF,)), dma((NF,)), dma((2,)), dma((2,)), dma((NH,)), dma((NH,)), dma((NH,)), dma((NH,)),
            dma((NF,)), dma((NF,)), dma((NF,)), dma((NF,)), dma((NF,)), dma((NF,)), dma((5,)),
        ],
        compiler_params=pltpu.CompilerParams(collective_id=0, has_side_effects=True),
        name="block_backward",
    )(x, dy, marks, wat, wct, tb)


def finish_kernel(gi_ref, attn_ref, conv_ref, out_ref, oattn_ref, oconv_ref):
    out_ref[...] = gi_ref[...]
    total = attn_ref[0]
    for i in range(1, NF):
        total = total + attn_ref[i]
    oattn_ref[...] = total
    for j in range(NF - 1):
        oconv_ref[12 * j : 12 * j + 12, :] = conv_ref[j].astype(F32)


def finish(gi, attn, conv):
    vm = pl.BlockSpec(memory_space=pltpu.VMEM)
    return pl.pallas_call(
        finish_kernel,
        out_shape=(
            jax.ShapeDtypeStruct((2, W, W, C), BF16),
            jax.ShapeDtypeStruct((5, C), F32),
            jax.ShapeDtypeStruct((180, C), F32),
        ),
        in_specs=[vm] * 3,
        out_specs=(vm, vm, vm),
        name="finish",
    )(gi, attn, conv)


def body(clip_latents, out_grad, box_mask, attn_weights, conv_weights, time_bias):
    got = block(clip_latents[0], out_grad[0], box_mask[0], attn_weights.T, conv_weights.T, time_bias)
    out, oattn, oconv = finish(*got)
    return out[None], oattn, oconv


def solution(mesh):
    in_specs = (
        P("dp", "frame", "height", None, None),
        P("dp", "frame", "height", None, None),
        P("dp", "frame", "height", None),
        P(),
        P(),
        P(),
    )
    out_specs = (
        P("dp", "frame", "height", None, None),
        P(("frame", "height", "dp"), None),
        P(("height", "dp"), None),
    )
    return jax.shard_map(body, mesh=mesh, in_specs=in_specs, out_specs=out_specs, check_vma=False)
```

```python
import jax
import jax.numpy as jnp
from jax import lax
from jax.experimental import pallas as pl
from jax.experimental.pallas import tpu as pltpu
from jax.sharding import PartitionSpec as P

F32 = jnp.float32
BF16 = jnp.bfloat16
GROUND_BIAS = 2.0
NF, NH, ND = 16, 8, 2
C = 320
PK = 640
HEADS = 5
T = 32
W = 16
ROWS = T * W
BLK = 128
NB = ROWS // BLK
NEG = -1e30
TOKENS = 2 * 32 * 128 * 16
GRAD_SCALE = float(TOKENS) ** -0.5
SCALING = 0.125


def peer(**where):
    return dict(device_id=where, device_id_type=pl.DeviceIdType.MESH)


def nn(a, b):
    return lax.dot_general(a, b, (((1,), (0,)), ((), ())), preferred_element_type=F32)


def nt(a, b):
    return lax.dot_general(a, b, (((1,), (1,)), ((), ())), preferred_element_type=F32)


def tn(a, b):
    return lax.dot_general(a, b, (((0,), (0,)), ((), ())), preferred_element_type=F32)


def pixel_major(src, tr, store):
    for s in range(5):
        tr[s, 0 : NF * W, :] = src[:, :, 128 * s : 128 * s + 128].reshape(NF * W, 128).astype(F32)
    for p in range(W):
        for e in range(2):
            for s in range(2):
                store(p, e, 128 * s, 128, tr[2 * e + s, pl.ds(p, NF, stride=W), :].astype(BF16))
            store(p, e, 256, 64, tr[4, pl.ds(p, NF, stride=W), :][:, 64 * e : 64 * e + 64].astype(BF16))


def pack(src, dst):
    for e in range(2):
        dst[:, :, 256 * e : 256 * e + 256] = src[e, :, :, 0:256]
    dst[:, :, 512:640] = jnp.concatenate([src[0, :, :, 256:320], src[1, :, :, 256:320]], axis=-1)


ORDER = (1, 15, 8, 2, 14, 7, 9, 3, 13, 6, 10, 4, 12, 5, 11)
SLABS = ((0, 128, (0, 1)), (128, 128, (2, 3)), (256, 64, (4,)))


def block_kernel(
    x_ref, dy_ref, mark_ref, wat_ref, wct_ref, tb_ref,
    out_ref, attn_cr, conv_dr,
    xs, ys, ms, mt, xt, dy0, dyu, dyd, wa, wc,
    tr, xp, dyp, q_s, k_s, v_s, o_s, pr, bias_s, y1_s, a_t, da_s, g_s, do_s, dq_s, dk_s, dv_s, x_t, o_t, cf,
    gi_s, attn_f, attn_l, conv_l, conv_a, attn_a, conv_1, attn_1, conv_b, attn_b, conv_f, conv_c, conv_cr, conv_d, attn_g, attn_c,
    mss, msr, xss, xsr, dss, dsr, hs, hr, gs, gr, pa, pb, cs, cr, as_, ar, c2s, c2r, c3s, c3r, a2s, a2r, lsem,
):
    f = lax.axis_index("frame")
    h = lax.axis_index("height")
    d = lax.axis_index("dp")
    other = 1 - d
    me = h * ND + d
    lin = h * NF + f
    prev = lax.rem(lin + NF * NH - 1, NF * NH)
    nxt = lax.rem(lin + 1, NF * NH)

    def remote(src, dst, ss, rs, **where):
        cp = pltpu.make_async_remote_copy(src_ref=src, dst_ref=dst, send_sem=ss, recv_sem=rs, **peer(**where))
        cp.start()
        return cp

    barrier = pltpu.get_barrier_semaphore()
    for k in range(1, NF):
        pl.semaphore_signal(barrier, inc=1, **peer(frame=lax.rem(f + k, NF)))
    for k in range(1, NH * ND):
        q = lax.rem(me + k, NH * ND)
        pl.semaphore_signal(barrier, inc=1, **peer(height=q // ND, dp=lax.rem(q, ND)))

    @pl.when(f == 0)
    def _():
        pl.semaphore_signal(barrier, inc=1, **peer(frame=lax.rem(prev, NF), height=prev // NF))

    @pl.when(f == NF - 1)
    def _():
        pl.semaphore_signal(barrier, inc=1, **peer(frame=lax.rem(nxt, NF), height=nxt // NF))

    lwa = pltpu.make_async_copy(wat_ref, wa, lsem.at[0])
    lwc = pltpu.make_async_copy(wct_ref, wc, lsem.at[1])
    lwa.start()
    lwc.start()

    pack(x_ref, xs)
    ms[:, 0, :] = jnp.zeros((NF, 128), F32)
    ms[:, 0, 0 : 2 * W] = jnp.concatenate([mark_ref[0], mark_ref[1]], axis=-1).astype(F32)
    pack(dy_ref, ys)

    edge = jnp.where(jnp.logical_or(f == 0, f == NF - 1), 1, 0)
    pl.semaphore_wait(barrier, NF + NH * ND - 2 + edge)

    xc, mc, dc = [], [], []
    for k in range(1, NF):
        p = lax.rem(f + k, NF)
        mc.append(remote(ms.at[p], mt.at[f], mss.at[k], msr.at[k], frame=p))
        xc.append(remote(xs.at[p], xt.at[f], xss.at[k], xsr.at[k], frame=p))
    for k in range(1, NF):
        p = lax.rem(f + k, NF)
        dc.append(remote(ys.at[p], dy0.at[f], dss.at[k], dsr.at[k], frame=p))
    lx = pltpu.make_async_copy(xs.at[f], xt.at[f], lsem.at[2])
    ld = pltpu.make_async_copy(ys.at[f], dy0.at[f], lsem.at[3])
    lm = pltpu.make_async_copy(ms.at[f], mt.at[f], lsem.at[5])
    lx.start()
    ld.start()
    lm.start()
    fwd = []

    def forward(k):
        part = lax.rem(f + NF - k, NF)
        up = remote(dy0.at[part], dyd.at[part], hs.at[0, k], hr.at[0, k], frame=lax.rem(prev, NF), height=prev // NF)
        down = remote(dy0.at[part], dyu.at[part], hs.at[1, k], hr.at[1, k], frame=lax.rem(nxt, NF), height=nxt // NF)
        fwd.append((up, down))

    ld.wait()
    forward(0)
    waiting = list(ORDER)

    def forward_next():
        if waiting:
            k = waiting.pop(0)
            dc[k - 1].wait_recv()
            forward(k)

    ri = lax.broadcasted_iota(jnp.int32, (BLK, BLK), 0) // T
    ci = lax.broadcasted_iota(jnp.int32, (BLK, BLK), 1) // T
    tq = lax.broadcasted_iota(jnp.int32, (T, T), 0)
    tu = lax.broadcasted_iota(jnp.int32, (T, T), 1)
    turn = jnp.where(tu == 2 * (tq & (NF - 1)) + (tq >> 4), 1.0, 0.0)

    def exact(left, right, dim):
        return lax.dot_general(
            left, right, (((1,), (dim,)), ((), ())), precision=lax.Precision.HIGHEST, preferred_element_type=F32
        )

    for hd in range(HEADS):
        one = exact(exact(turn, tb_ref[hd], 0), turn, 1)
        wide = jnp.concatenate([one] * 4, axis=1)
        full = jnp.concatenate([wide] * 4, axis=0)
        bias_s[hd] = jnp.where(ri == ci, full, NEG)
    zero = jnp.zeros((T, C), BF16)
    for r in range(3):
        dyp[r, 0:T, :] = zero
        dyp[r, (W + 1) * T :, :] = zero
    lane = lax.broadcasted_iota(jnp.int32, (BLK, 128), 1)
    low = lane < 64
    ones = jnp.full((8, 128), GROUND_BIAS, BF16)

    def only(val, i, w):
        if w == 64:
            return val
        keep = low if i == 0 else jnp.logical_not(low)
        return jnp.where(keep, val, jnp.zeros_like(val))

    def pick(parts, w):
        if w == 64:
            return parts[0]
        return jnp.where(low, parts[0], parts[1])

    lwa.wait()
    lx.wait()
    lm.wait()
    for k in ORDER:
        mc[k - 1].wait_recv()
        xc[k - 1].wait_recv()

    def put_x(p, e, s, w, val):
        xp[p * T + e * NF : p * T + (e + 1) * NF, s : s + w] = val

    pixel_major(xt, tr, put_x)
    x = xp[...]
    marks_all = jnp.concatenate([mt[:, 0, :]] * 8, axis=0)
    row_b = lax.broadcasted_iota(jnp.int32, (BLK, 128), 0)
    home = ((row_b >> 4) & 1) * W + (row_b >> 5)
    q_s[...] = nt(x, wa[:, 0:C]).astype(BF16)
    k_s[...] = nt(x, wa[:, C : 2 * C]).astype(BF16)
    v_s[...] = nt(x, wa[:, 2 * C : 3 * C]).astype(BF16)

    for b in range(NB):
        rows = slice(b * BLK, (b + 1) * BLK)
        marks = jnp.where(lane == home + 4 * b, marks_all, 0.0).astype(BF16)
        key_bias = nt(ones, marks)[0:1, :]
        for s, w, heads in SLABS:
            ls = slice(s, s + w)
            qb, kb, vb = q_s[rows, ls], k_s[rows, ls], v_s[rows, ls]
            outs = []
            for i, hd in enumerate(heads):
                sc = nt(only(qb, i, w), kb) * SCALING + bias_s[hd] + key_bias
                e = jnp.exp(sc - jnp.max(sc, axis=-1, keepdims=True))
                pf = e / jnp.sum(e, axis=-1, keepdims=True)
                pr[b, hd] = pf
                outs.append(nn(pf.astype(BF16), vb))
            o_s[rows, ls] = pick(outs, w).astype(BF16)
            forward_next()
    while waiting:
        forward_next()

    y1 = (x.astype(F32) + nt(o_s[...], wa[:, 3 * C :])).astype(BF16)
    y1_s[...] = y1
    yf = y1.astype(F32)
    act = yf / (1.0 + jnp.exp(-yf))
    a_t[...] = act.T.astype(BF16)

    def place_row(r, src, keep):
        def put(p, e, s, w, val):
            if keep is not None:
                val = jnp.where(keep, val, jnp.zeros_like(val))
            at = (p + 1) * T + e * NF
            dyp[r, at : at + NF, s : s + w] = val

        pixel_major(src, tr, put)

    def tap_row(r, first):
        for c in range(3):
            tap = 3 * r + c
            off = (2 - c) * T
            shifted = dyp[r, off : off + ROWS, :]
            part = nn(shifted, wc[:, tap * C : (tap + 1) * C])
            da_s[...] = part if first else da_s[...] + part
            first = False
            cf[tap * C : (tap + 1) * C, :] = nn(a_t[...], shifted) * GRAD_SCALE

    lwc.wait()
    place_row(1, dy0, None)
    tap_row(1, True)
    rr = lax.broadcasted_iota(jnp.int32, (C, C), 0)
    cc_ = lax.broadcasted_iota(jnp.int32, (C, C), 1)
    mm = (rr * 3277) >> 16
    rem = rr - 20 * mm
    cf_ = (rem * 13108) >> 16
    perm = jnp.where(cc_ == 80 * cf_ + 5 * mm + (rem - 5 * cf_), 1.0, 0.0).astype(BF16)
    x_t[...] = nt(perm, x).astype(BF16)
    o_t[...] = nt(perm, o_s[...]).astype(BF16)
    for up, _ in fwd:
        up.wait_recv()
    place_row(0, dyd, lin < NF * NH - 1)
    tap_row(0, False)
    for _, down in fwd:
        down.wait_recv()
    place_row(2, dyu, lin > 0)
    tap_row(2, False)

    for k in range(NH * ND):
        conv_l[k // ND, k % ND] = cf[k * 180 : (k + 1) * 180, :].astype(BF16)
    ca = remote(conv_l.at[:, other], conv_a, pa.at[0], pb.at[0], dp=other)

    yf = y1_s[...].astype(F32)
    sig = 1.0 / (1.0 + jnp.exp(-yf))
    slope = sig * (1.0 + yf * (1.0 - sig))
    g = (dyp[1, T : T + ROWS, :].astype(F32) + slope * da_s[...]).astype(BF16)
    g_s[...] = g
    do_s[...] = nn(g, wa[:, 3 * C :]).astype(BF16)

    def attn_term(j, left, right):
        term = nn(left[...], right[...]) * GRAD_SCALE
        for m in range(NH * ND):
            attn_f[m, 20 * j : 20 * j + 20, :] = term[20 * m : 20 * m + 20, :]

    attn_term(3, o_t, g_s)
    ca.wait_recv()
    for j in range(NH):
        conv_1[j] = (conv_l[j, d].astype(F32) + conv_a[j].astype(F32)).astype(BF16)
    cc = []
    for k in range(1, NH):
        p = lax.rem(h + k, NH)
        cc.append(remote(conv_1.at[p], conv_b.at[k], cs.at[k], cr.at[k], height=p))

    for b in range(NB):
        rows = slice(b * BLK, (b + 1) * BLK)
        for s, w, heads in SLABS:
            ls = slice(s, s + w)
            qb, kb, vb, db = q_s[rows, ls], k_s[rows, ls], v_s[rows, ls], do_s[rows, ls]
            dqs, dks, dvs = [], [], []
            for i, hd in enumerate(heads):
                pf = pr[b, hd]
                dp = nt(only(db, i, w), vb)
                dsc = (pf * (dp - jnp.sum(pf * dp, axis=-1, keepdims=True))).astype(BF16)
                dqs.append(nn(dsc, kb))
                dks.append(tn(dsc, qb))
                dvs.append(tn(pf.astype(BF16), db))
            dq_s[rows, ls] = (pick(dqs, w) * SCALING).astype(BF16)
            dk_s[rows, ls] = (pick(dks, w) * SCALING).astype(BF16)
            dv_s[rows, ls] = pick(dvs, w).astype(BF16)

    for j, right in enumerate((dq_s, dk_s, dv_s)):
        attn_term(j, x_t, right)
    for m in range(NH * ND):
        attn_l[m // ND, m % ND] = attn_f[m].astype(BF16)
    aa = remote(attn_l.at[:, other], attn_a, pa.at[1], pb.at[1], dp=other)

    dx = nn(dq_s[...], wa[:, 0:C]) + nn(dk_s[...], wa[:, C : 2 * C]) + nn(dv_s[...], wa[:, 2 * C : 3 * C])
    gi = g_s[...].astype(F32) + dx.astype(BF16).astype(F32)
    for s in range(2):
        tr[s] = gi[:, 128 * s : 128 * s + 128]
    tr[2, :, 0:64] = gi[:, 256:320]
    for t in range(NF):
        for e in range(2):
            for s in range(2):
                at = 256 * e + 128 * s
                gi_s[t, :, at : at + 128] = tr[s, pl.ds(e * NF + t, W, stride=T), :].astype(BF16)
        ends = [tr[2, pl.ds(e * NF + t, W, stride=T), :][:, 0:64] for e in range(2)]
        gi_s[t, :, 512:640] = jnp.concatenate(ends, axis=-1).astype(BF16)
    gic = []
    for k in range(1, NF):
        p = lax.rem(f + k, NF)
        gic.append(remote(gi_s.at[p], out_ref.at[f], gs.at[k], gr.at[k], frame=p))
    own = pltpu.make_async_copy(gi_s.at[f], out_ref.at[f], lsem.at[4])
    own.start()

    aa.wait_recv()
    for j in range(NH):
        attn_1[j] = (attn_l[j, d].astype(F32) + attn_a[j].astype(F32)).astype(BF16)
    ac = []
    for k in range(1, NH):
        p = lax.rem(h + k, NH)
        ac.append(remote(attn_1.at[p], attn_b.at[k], as_.at[k], ar.at[k], height=p))

    total = conv_1[h].astype(F32)
    for k in range(1, NH):
        cc[k - 1].wait_recv()
        total = total + conv_b[k].astype(F32)
    conv_f[0:180, :] = total
    conv_f[180:192, :] = jnp.zeros((12, C), F32)
    for j in range(NF):
        conv_c[j] = conv_f[12 * j : 12 * j + 12, :].astype(BF16)
    c2 = []
    for k in range(1, NF):
        p = lax.rem(f + k, NF)
        c2.append(remote(conv_c.at[p], conv_cr.at[k], c2s.at[k], c2r.at[k], frame=p))

    total = attn_1[h].astype(F32)
    for k in range(1, NH):
        ac[k - 1].wait_recv()
        total = total + attn_b[k].astype(F32)
    attn_g[...] = total
    for j in range(NF):
        attn_c[j] = attn_g[5 * j : 5 * j + 5, :]
    a2 = []
    for k in range(1, NF):
        p = lax.rem(f + k, NF)
        a2.append(remote(attn_c.at[p], attn_cr.at[k], a2s.at[k], a2r.at[k], frame=p))
    attn_cr[0] = attn_c[f]

    total = conv_c[f].astype(F32)
    for k in range(1, NF):
        c2[k - 1].wait_recv()
        total = total + conv_cr[k].astype(F32)
    conv_d[...] = total.astype(BF16)
    c3 = []
    for k in range(1, NF):
        p = lax.rem(f + k, NF)
        c3.append(remote(conv_d, conv_dr.at[f], c3s.at[k], c3r.at[k], frame=p))
    conv_dr[f] = total.astype(BF16)

    own.wait()
    for cp in a2 + c3 + gic:
        cp.wait_recv()
    for cp in mc + xc + dc + [ca, aa] + gic + cc + ac + a2 + c2 + c3:
        cp.wait_send()
    for up, down in fwd:
        up.wait_send()
        down.wait_send()


def block(x, dy, marks, wat, wct, tb):
    vm = pl.BlockSpec(memory_space=pltpu.VMEM)
    anyw = pl.BlockSpec(memory_space=pl.ANY)
    v = pltpu.VMEM
    dma = pltpu.SemaphoreType.DMA
    tok = v((ROWS, C), BF16)
    row = v((NF, W, PK), BF16)
    mark = v((NF, 1, 128), F32)
    return pl.pallas_call(
        block_kernel,
        out_shape=(
            jax.ShapeDtypeStruct((W, W, PK), BF16),
            jax.ShapeDtypeStruct((NF, 5, C), F32),
            jax.ShapeDtypeStruct((NF, 12, C), BF16),
        ),
        in_specs=[vm, vm, vm, anyw, anyw, vm],
        out_specs=(vm, vm, vm),
        scratch_shapes=[
            row, row, mark, mark, row, row, row, row, v((C, 4 * C), BF16), v((C, 9 * C), BF16),
            v((5, ROWS, 128), F32), v((ROWS, C), BF16), v((3, ROWS + 2 * T, C), BF16),
            tok, tok, tok, tok,
            v((NB, HEADS, BLK, BLK), F32), v((HEADS, BLK, BLK), F32),
            tok, v((C, ROWS), BF16), v((ROWS, C), F32), tok, tok, tok, tok, tok,
            v((C, ROWS), BF16), v((C, ROWS), BF16), v((9 * C, C), F32),
            row, v((NH * ND, 80, C), F32), v((NH, ND, 80, C), BF16), v((NH, ND, 180, C), BF16),
            v((NH, 180, C), BF16), v((NH, 80, C), BF16), v((NH, 180, C), BF16), v((NH, 80, C), BF16),
            v((NH, 180, C), BF16), v((NH, 80, C), BF16), v((192, C), F32), v((NF, 12, C), BF16), v((NF, 12, C), BF16),
            v((12, C), BF16), v((80, C), F32), v((NF, 5, C), F32),
            dma((NF,)), dma((NF,)), dma((NF,)), dma((NF,)), dma((NF,)), dma((NF,)), dma((2, NF)), dma((2, NF)),
            dma((NF,)), dma((NF,)), dma((2,)), dma((2,)), dma((NH,)), dma((NH,)), dma((NH,)), dma((NH,)),
            dma((NF,)), dma((NF,)), dma((NF,)), dma((NF,)), dma((NF,)), dma((NF,)), dma((6,)),
        ],
        compiler_params=pltpu.CompilerParams(collective_id=0, has_side_effects=True),
        name="block_backward",
    )(x, dy, marks, wat, wct, tb)


def finish_kernel(gi_ref, attn_ref, conv_ref, out_ref, oattn_ref, oconv_ref):
    for e in range(2):
        out_ref[e, :, :, 0:256] = gi_ref[:, :, 256 * e : 256 * e + 256]
        out_ref[e, :, :, 256:320] = gi_ref[:, :, 512 + 64 * e : 576 + 64 * e]
    total = attn_ref[0]
    for i in range(1, NF):
        total = total + attn_ref[i]
    oattn_ref[...] = total
    for j in range(NF - 1):
        oconv_ref[12 * j : 12 * j + 12, :] = conv_ref[j].astype(F32)


def finish(gi, attn, conv):
    vm = pl.BlockSpec(memory_space=pltpu.VMEM)
    return pl.pallas_call(
        finish_kernel,
        out_shape=(
            jax.ShapeDtypeStruct((2, W, W, C), BF16),
            jax.ShapeDtypeStruct((5, C), F32),
            jax.ShapeDtypeStruct((180, C), F32),
        ),
        in_specs=[vm] * 3,
        out_specs=(vm, vm, vm),
        name="finish",
    )(gi, attn, conv)


def body(clip_latents, out_grad, box_mask, attn_weights, conv_weights, time_bias):
    got = block(clip_latents[0], out_grad[0], box_mask[0], attn_weights.T, conv_weights.T, time_bias)
    out, oattn, oconv = finish(*got)
    return out[None], oattn, oconv


def solution(mesh):
    in_specs = (
        P("dp", "frame", "height", None, None),
        P("dp", "frame", "height", None, None),
        P("dp", "frame", "height", None),
        P(),
        P(),
        P(),
    )
    out_specs = (
        P("dp", "frame", "height", None, None),
        P(("frame", "height", "dp"), None),
        P(("height", "dp"), None),
    )
    return jax.shard_map(body, mesh=mesh, in_specs=in_specs, out_specs=out_specs, check_vma=False)
```

```python
import jax
import jax.numpy as jnp
from jax import lax
from jax.experimental import pallas as pl
from jax.experimental.pallas import tpu as pltpu
from jax.sharding import PartitionSpec as P

F32 = jnp.float32
BF16 = jnp.bfloat16
GROUND_BIAS = 2.0
NF, NH, ND = 16, 8, 2
C = 320
PK = 640
HEADS = 5
T = 32
W = 16
ROWS = T * W
BLK = 128
NB = ROWS // BLK
NEG = -1e30
TOKENS = 2 * 32 * 128 * 16
GRAD_SCALE = float(TOKENS) ** -0.5
SCALING = 0.125


def peer(**where):
    return dict(device_id=where, device_id_type=pl.DeviceIdType.MESH)


def nn(a, b):
    return lax.dot_general(a, b, (((1,), (0,)), ((), ())), preferred_element_type=F32)


def nt(a, b):
    return lax.dot_general(a, b, (((1,), (1,)), ((), ())), preferred_element_type=F32)


def tn(a, b):
    return lax.dot_general(a, b, (((0,), (0,)), ((), ())), preferred_element_type=F32)


def pixel_major(src, tr, store):
    for s in range(5):
        tr[s, 0 : NF * W, :] = src[:, :, 128 * s : 128 * s + 128].reshape(NF * W, 128).astype(F32)
    for p in range(W):
        for e in range(2):
            for s in range(2):
                store(p, e, 128 * s, 128, tr[2 * e + s, pl.ds(p, NF, stride=W), :].astype(BF16))
            store(p, e, 256, 64, tr[4, pl.ds(p, NF, stride=W), :][:, 64 * e : 64 * e + 64].astype(BF16))


def pack(src, dst):
    for e in range(2):
        dst[:, :, 256 * e : 256 * e + 256] = src[e, :, :, 0:256]
    dst[:, :, 512:640] = jnp.concatenate([src[0, :, :, 256:320], src[1, :, :, 256:320]], axis=-1)


ORDER = (1, 15, 8, 2, 14, 7, 9, 3, 13, 6, 10, 4, 12, 5, 11)
SLABS = ((0, 128, (0, 1)), (128, 128, (2, 3)), (256, 64, (4,)))


def block_kernel(
    x_ref, dy_ref, mark_ref, wat_ref, wct_ref, tb_ref,
    out_ref, attn_cr, conv_dr,
    xs, ys, ms, mt, xt, dy0, dyu, dyd, wa, wc,
    tr, xp, dyp, q_s, k_s, v_s, o_s, pr, bias_s, y1_s, a_t, da_s, g_s, do_s, dq_s, dk_s, dv_s, x_t, o_t, cf,
    gi_s, attn_f, attn_l, conv_l, conv_a, attn_a, conv_1, attn_1, conv_b, attn_b, conv_f, conv_c, conv_cr, conv_d, attn_g, attn_w, attn_c,
    mss, msr, xss, xsr, dss, dsr, hs, hr, gs, gr, pa, pb, cs, cr, as_, ar, c2s, c2r, c3s, c3r, a2s, a2r, lsem,
):
    f = lax.axis_index("frame")
    h = lax.axis_index("height")
    d = lax.axis_index("dp")
    other = 1 - d
    me = h * ND + d
    lin = h * NF + f
    prev = lax.rem(lin + NF * NH - 1, NF * NH)
    nxt = lax.rem(lin + 1, NF * NH)

    def remote(src, dst, ss, rs, **where):
        cp = pltpu.make_async_remote_copy(src_ref=src, dst_ref=dst, send_sem=ss, recv_sem=rs, **peer(**where))
        cp.start()
        return cp

    barrier = pltpu.get_barrier_semaphore()
    for k in range(1, NF):
        pl.semaphore_signal(barrier, inc=1, **peer(frame=lax.rem(f + k, NF)))
    for k in range(1, NH * ND):
        q = lax.rem(me + k, NH * ND)
        pl.semaphore_signal(barrier, inc=1, **peer(height=q // ND, dp=lax.rem(q, ND)))

    @pl.when(f == 0)
    def _():
        pl.semaphore_signal(barrier, inc=1, **peer(frame=lax.rem(prev, NF), height=prev // NF))

    @pl.when(f == NF - 1)
    def _():
        pl.semaphore_signal(barrier, inc=1, **peer(frame=lax.rem(nxt, NF), height=nxt // NF))

    lwa = pltpu.make_async_copy(wat_ref, wa, lsem.at[0])
    lwc = pltpu.make_async_copy(wct_ref, wc, lsem.at[1])
    lwa.start()
    lwc.start()

    pack(x_ref, xs)
    ms[:, 0, :] = jnp.zeros((NF, 128), F32)
    ms[:, 0, 0 : 2 * W] = jnp.concatenate([mark_ref[0], mark_ref[1]], axis=-1).astype(F32)
    pack(dy_ref, ys)

    edge = jnp.where(jnp.logical_or(f == 0, f == NF - 1), 1, 0)
    pl.semaphore_wait(barrier, NF + NH * ND - 2 + edge)

    xc, mc, dc = [], [], []
    for k in range(1, NF):
        p = lax.rem(f + k, NF)
        mc.append(remote(ms.at[p], mt.at[f], mss.at[k], msr.at[k], frame=p))
        xc.append(remote(xs.at[p], xt.at[f], xss.at[k], xsr.at[k], frame=p))
    for k in range(1, NF):
        p = lax.rem(f + k, NF)
        dc.append(remote(ys.at[p], dy0.at[f], dss.at[k], dsr.at[k], frame=p))
    lx = pltpu.make_async_copy(xs.at[f], xt.at[f], lsem.at[2])
    ld = pltpu.make_async_copy(ys.at[f], dy0.at[f], lsem.at[3])
    lm = pltpu.make_async_copy(ms.at[f], mt.at[f], lsem.at[5])
    lx.start()
    ld.start()
    lm.start()
    fwd = []

    def forward(k):
        part = lax.rem(f + NF - k, NF)
        up = remote(dy0.at[part], dyd.at[part], hs.at[0, k], hr.at[0, k], frame=lax.rem(prev, NF), height=prev // NF)
        down = remote(dy0.at[part], dyu.at[part], hs.at[1, k], hr.at[1, k], frame=lax.rem(nxt, NF), height=nxt // NF)
        fwd.append((up, down))

    ld.wait()
    forward(0)
    waiting = list(ORDER)

    def forward_next():
        if waiting:
            k = waiting.pop(0)
            dc[k - 1].wait_recv()
            forward(k)

    ri = lax.broadcasted_iota(jnp.int32, (BLK, BLK), 0) // T
    ci = lax.broadcasted_iota(jnp.int32, (BLK, BLK), 1) // T
    tq = lax.broadcasted_iota(jnp.int32, (T, T), 0)
    tu = lax.broadcasted_iota(jnp.int32, (T, T), 1)
    turn = jnp.where(tu == 2 * (tq & (NF - 1)) + (tq >> 4), 1.0, 0.0)

    def exact(left, right, dim):
        return lax.dot_general(
            left, right, (((1,), (dim,)), ((), ())), precision=lax.Precision.HIGHEST, preferred_element_type=F32
        )

    for hd in range(HEADS):
        one = exact(exact(turn, tb_ref[hd], 0), turn, 1)
        wide = jnp.concatenate([one] * 4, axis=1)
        full = jnp.concatenate([wide] * 4, axis=0)
        bias_s[hd] = jnp.where(ri == ci, full, NEG)
    conv_l[...] = jnp.zeros_like(conv_l)
    attn_f[...] = jnp.zeros_like(attn_f)
    attn_w[...] = jnp.zeros_like(attn_w)
    zero = jnp.zeros((T, C), BF16)
    for r in range(3):
        dyp[r, 0:T, :] = zero
        dyp[r, (W + 1) * T :, :] = zero
    lane = lax.broadcasted_iota(jnp.int32, (BLK, 128), 1)
    low = lane < 64
    ones = jnp.full((8, 128), GROUND_BIAS, BF16)

    def only(val, i, w):
        if w == 64:
            return val
        keep = low if i == 0 else jnp.logical_not(low)
        return jnp.where(keep, val, jnp.zeros_like(val))

    def pick(parts, w):
        if w == 64:
            return parts[0]
        return jnp.where(low, parts[0], parts[1])

    lwa.wait()
    lx.wait()
    lm.wait()
    for k in ORDER:
        mc[k - 1].wait_recv()
        xc[k - 1].wait_recv()

    def put_x(p, e, s, w, val):
        xp[p * T + e * NF : p * T + (e + 1) * NF, s : s + w] = val

    pixel_major(xt, tr, put_x)
    x = xp[...]
    marks_all = jnp.concatenate([mt[:, 0, :]] * 8, axis=0)
    row_b = lax.broadcasted_iota(jnp.int32, (BLK, 128), 0)
    home = ((row_b >> 4) & 1) * W + (row_b >> 5)
    q_s[...] = nt(x, wa[:, 0:C]).astype(BF16)
    k_s[...] = nt(x, wa[:, C : 2 * C]).astype(BF16)
    v_s[...] = nt(x, wa[:, 2 * C : 3 * C]).astype(BF16)

    for b in range(NB):
        rows = slice(b * BLK, (b + 1) * BLK)
        marks = jnp.where(lane == home + 4 * b, marks_all, 0.0).astype(BF16)
        key_bias = nt(ones, marks)[0:1, :]
        for s, w, heads in SLABS:
            ls = slice(s, s + w)
            qb, kb, vb = q_s[rows, ls], k_s[rows, ls], v_s[rows, ls]
            outs = []
            for i, hd in enumerate(heads):
                sc = nt(only(qb, i, w), kb) * SCALING + bias_s[hd] + key_bias
                e = jnp.exp(sc - jnp.max(sc, axis=-1, keepdims=True))
                pf = e / jnp.sum(e, axis=-1, keepdims=True)
                pr[b, hd] = pf
                outs.append(nn(pf.astype(BF16), vb))
            o_s[rows, ls] = pick(outs, w).astype(BF16)
            forward_next()
    while waiting:
        forward_next()

    y1 = (x.astype(F32) + nt(o_s[...], wa[:, 3 * C :])).astype(BF16)
    y1_s[...] = y1
    yf = y1.astype(F32)
    act = yf / (1.0 + jnp.exp(-yf))
    a_t[...] = act.T.astype(BF16)

    def place_row(r, src, keep):
        def put(p, e, s, w, val):
            if keep is not None:
                val = jnp.where(keep, val, jnp.zeros_like(val))
            at = (p + 1) * T + e * NF
            dyp[r, at : at + NF, s : s + w] = val

        pixel_major(src, tr, put)

    def tap_row(r, first):
        for c in range(3):
            tap = 3 * r + c
            off = (2 - c) * T
            shifted = dyp[r, off : off + ROWS, :]
            part = nn(shifted, wc[:, tap * C : (tap + 1) * C])
            da_s[...] = part if first else da_s[...] + part
            first = False
            cf[tap * C : (tap + 1) * C, :] = nn(a_t[...], shifted) * GRAD_SCALE

    lwc.wait()
    place_row(1, dy0, None)
    tap_row(1, True)
    rr = lax.broadcasted_iota(jnp.int32, (C, C), 0)
    cc_ = lax.broadcasted_iota(jnp.int32, (C, C), 1)
    mm = (rr * 3277) >> 16
    rem = rr - 20 * mm
    cf_ = (rem * 13108) >> 16
    perm = jnp.where(cc_ == 80 * cf_ + 5 * mm + (rem - 5 * cf_), 1.0, 0.0).astype(BF16)
    x_t[...] = nt(perm, x).astype(BF16)
    o_t[...] = nt(perm, o_s[...]).astype(BF16)
    for up, _ in fwd:
        up.wait_recv()
    place_row(0, dyd, lin < NF * NH - 1)
    tap_row(0, False)

    def halve(first, last, i):
        for k in range(ND * first, ND * last):
            at = 180 * k
            to = conv_l.at[k // ND, k % ND]
            to[0:180, :] = cf[at : at + 180, 0:128].astype(BF16)
            to[192:372, :] = cf[at : at + 180, 128:256].astype(BF16)
            ends = [cf[at : at + 90, 256:320], cf[at + 90 : at + 180, 256:320]]
            to[384:474, :] = jnp.concatenate(ends, axis=-1).astype(BF16)
        part = pl.ds(first, last - first)
        return remote(conv_l.at[part, other], conv_a.at[part], pa.at[i], pb.at[i], dp=other)

    cc = []
    for k in range(1, NH):
        cc.append(
            pltpu.make_async_remote_copy(
                src_ref=conv_1.at[lax.rem(h + k, NH)],
                dst_ref=conv_b.at[k],
                send_sem=cs.at[k],
                recv_sem=cr.at[k],
                **peer(height=lax.rem(h + k, NH)),
            )
        )

    def spread(first, last):
        for j in range(first, last):
            conv_1[j] = (conv_l[j, d].astype(F32) + conv_a[j].astype(F32)).astype(BF16)
        for k in range(1, NH):
            p = lax.rem(h + k, NH)

            @pl.when(jnp.logical_and(p >= first, p < last))
            def _(k=k):
                cc[k - 1].start()

    ca = halve(0, 5, 0)
    for _, down in fwd:
        down.wait_recv()
    place_row(2, dyu, lin > 0)
    tap_row(2, False)
    cb = halve(5, NH, 2)
    ca.wait_recv()
    spread(0, 5)

    yf = y1_s[...].astype(F32)
    sig = 1.0 / (1.0 + jnp.exp(-yf))
    slope = sig * (1.0 + yf * (1.0 - sig))
    g = (dyp[1, T : T + ROWS, :].astype(F32) + slope * da_s[...]).astype(BF16)
    g_s[...] = g
    do_s[...] = nn(g, wa[:, 3 * C :]).astype(BF16)

    def attn_term(j, left, right):
        term = nn(left[...], right[...]) * GRAD_SCALE
        for m in range(NH * ND):
            piece = term[20 * m : 20 * m + 20, :]
            attn_f[m, 20 * j : 20 * j + 20, :] = piece[:, 0:128]
            attn_f[m, 80 + 20 * j : 100 + 20 * j, :] = piece[:, 128:256]
            attn_f[m, 160 + 10 * j : 170 + 10 * j, :] = jnp.concatenate([piece[0:10, 256:], piece[10:20, 256:]], axis=-1)

    cb.wait_recv()
    spread(5, NH)
    attn_term(3, o_t, g_s)

    for b in range(NB):
        rows = slice(b * BLK, (b + 1) * BLK)
        for s, w, heads in SLABS:
            ls = slice(s, s + w)
            qb, kb, vb, db = q_s[rows, ls], k_s[rows, ls], v_s[rows, ls], do_s[rows, ls]
            dqs, dks, dvs = [], [], []
            for i, hd in enumerate(heads):
                pf = pr[b, hd]
                dp = nt(only(db, i, w), vb)
                dsc = (pf * (dp - jnp.sum(pf * dp, axis=-1, keepdims=True))).astype(BF16)
                dqs.append(nn(dsc, kb))
                dks.append(tn(dsc, qb))
                dvs.append(tn(pf.astype(BF16), db))
            dq_s[rows, ls] = (pick(dqs, w) * SCALING).astype(BF16)
            dk_s[rows, ls] = (pick(dks, w) * SCALING).astype(BF16)
            dv_s[rows, ls] = pick(dvs, w).astype(BF16)

    for j, right in enumerate((dq_s, dk_s, dv_s)):
        attn_term(j, x_t, right)
    for m in range(NH * ND):
        attn_l[m // ND, m % ND] = attn_f[m].astype(BF16)
    aa = remote(attn_l.at[:, other], attn_a, pa.at[1], pb.at[1], dp=other)

    dx = nn(dq_s[...], wa[:, 0:C]) + nn(dk_s[...], wa[:, C : 2 * C]) + nn(dv_s[...], wa[:, 2 * C : 3 * C])
    gi = g_s[...].astype(F32) + dx.astype(BF16).astype(F32)
    for s in range(2):
        tr[s] = gi[:, 128 * s : 128 * s + 128]
    tr[2, :, 0:64] = gi[:, 256:320]
    for t in range(NF):
        for e in range(2):
            for s in range(2):
                at = 256 * e + 128 * s
                gi_s[t, :, at : at + 128] = tr[s, pl.ds(e * NF + t, W, stride=T), :].astype(BF16)
        ends = [tr[2, pl.ds(e * NF + t, W, stride=T), :][:, 0:64] for e in range(2)]
        gi_s[t, :, 512:640] = jnp.concatenate(ends, axis=-1).astype(BF16)
    gic = []
    for k in range(1, NF):
        p = lax.rem(f + k, NF)
        gic.append(remote(gi_s.at[p], out_ref.at[f], gs.at[k], gr.at[k], frame=p))
    own = pltpu.make_async_copy(gi_s.at[f], out_ref.at[f], lsem.at[4])
    own.start()

    aa.wait_recv()
    for j in range(NH):
        attn_1[j] = (attn_l[j, d].astype(F32) + attn_a[j].astype(F32)).astype(BF16)
    ac = []
    for k in range(1, NH):
        p = lax.rem(h + k, NH)
        ac.append(remote(attn_1.at[p], attn_b.at[k], as_.at[k], ar.at[k], height=p))

    total = conv_1[h].astype(F32)
    for k in range(1, NH):
        cc[k - 1].wait_recv()
        total = total + conv_b[k].astype(F32)
    conv_f[0:480, :] = total
    conv_f[480:512, :] = jnp.zeros((32, 128), F32)
    for j in range(NF):
        conv_c[j] = conv_f[32 * j : 32 * j + 32, :].astype(BF16)
    c2 = []
    for k in range(1, NF):
        p = lax.rem(f + k, NF)
        c2.append(remote(conv_c.at[p], conv_cr.at[k], c2s.at[k], c2r.at[k], frame=p))

    total = attn_1[h].astype(F32)
    for k in range(1, NH):
        ac[k - 1].wait_recv()
        total = total + attn_b[k].astype(F32)
    attn_g[...] = total
    for j in range(NF):
        at = 160 + 10 * (j // 4) + 5 * (j % 2)
        to = 64 * (j % 4 // 2)
        attn_w[j, 0:5, :] = attn_g[5 * j : 5 * j + 5, :]
        attn_w[j, 5:10, :] = attn_g[80 + 5 * j : 85 + 5 * j, :]
        attn_w[j, 10:15, 0:64] = attn_g[at : at + 5, to : to + 64]
    for j in range(NF):
        attn_c[j] = attn_w[j].astype(BF16)
    a2 = []
    for k in range(1, NF):
        p = lax.rem(f + k, NF)
        a2.append(remote(attn_c.at[p], attn_cr.at[k], a2s.at[k], a2r.at[k], frame=p))
    attn_cr[0] = attn_c[f]

    total = conv_c[f].astype(F32)
    for k in range(1, NF):
        c2[k - 1].wait_recv()
        total = total + conv_cr[k].astype(F32)
    conv_d[...] = total.astype(BF16)
    c3 = []
    for k in range(1, NF):
        p = lax.rem(f + k, NF)
        c3.append(remote(conv_d, conv_dr.at[f], c3s.at[k], c3r.at[k], frame=p))
    conv_dr[f] = total.astype(BF16)

    own.wait()
    for cp in a2 + c3 + gic:
        cp.wait_recv()
    for cp in mc + xc + dc + [ca, cb, aa] + gic + cc + ac + a2 + c2 + c3:
        cp.wait_send()
    for up, down in fwd:
        up.wait_send()
        down.wait_send()


def block(x, dy, marks, wat, wct, tb):
    vm = pl.BlockSpec(memory_space=pltpu.VMEM)
    anyw = pl.BlockSpec(memory_space=pl.ANY)
    v = pltpu.VMEM
    dma = pltpu.SemaphoreType.DMA
    tok = v((ROWS, C), BF16)
    row = v((NF, W, PK), BF16)
    mark = v((NF, 1, 128), F32)
    return pl.pallas_call(
        block_kernel,
        out_shape=(
            jax.ShapeDtypeStruct((W, W, PK), BF16),
            jax.ShapeDtypeStruct((NF, 16, 128), BF16),
            jax.ShapeDtypeStruct((NF, 32, 128), BF16),
        ),
        in_specs=[vm, vm, vm, anyw, anyw, vm],
        out_specs=(vm, vm, vm),
        scratch_shapes=[
            row, row, mark, mark, row, row, row, row, v((C, 4 * C), BF16), v((C, 9 * C), BF16),
            v((5, ROWS, 128), F32), v((ROWS, C), BF16), v((3, ROWS + 2 * T, C), BF16),
            tok, tok, tok, tok,
            v((NB, HEADS, BLK, BLK), F32), v((HEADS, BLK, BLK), F32),
            tok, v((C, ROWS), BF16), v((ROWS, C), F32), tok, tok, tok, tok, tok,
            v((C, ROWS), BF16), v((C, ROWS), BF16), v((9 * C, C), F32),
            row, v((NH * ND, 208, 128), F32), v((NH, ND, 208, 128), BF16), v((NH, ND, 480, 128), BF16),
            v((NH, 480, 128), BF16), v((NH, 208, 128), BF16), v((NH, 480, 128), BF16), v((NH, 208, 128), BF16),
            v((NH, 480, 128), BF16), v((NH, 208, 128), BF16),
            v((512, 128), F32), v((NF, 32, 128), BF16), v((NF, 32, 128), BF16), v((32, 128), BF16),
            v((208, 128), F32), v((NF, 16, 128), F32), v((NF, 16, 128), BF16),
            dma((NF,)), dma((NF,)), dma((NF,)), dma((NF,)), dma((NF,)), dma((NF,)), dma((2, NF)), dma((2, NF)),
            dma((NF,)), dma((NF,)), dma((3,)), dma((3,)), dma((NH,)), dma((NH,)), dma((NH,)), dma((NH,)),
            dma((NF,)), dma((NF,)), dma((NF,)), dma((NF,)), dma((NF,)), dma((NF,)), dma((6,)),
        ],
        compiler_params=pltpu.CompilerParams(collective_id=0, has_side_effects=True),
        name="block_backward",
    )(x, dy, marks, wat, wct, tb)


def finish_kernel(gi_ref, attn_ref, conv_ref, out_ref, oattn_ref, oconv_ref):
    for e in range(2):
        out_ref[e, :, :, 0:256] = gi_ref[:, :, 256 * e : 256 * e + 256]
        out_ref[e, :, :, 256:320] = gi_ref[:, :, 512 + 64 * e : 576 + 64 * e]
    total = attn_ref[0].astype(F32)
    for i in range(1, NF):
        total = total + attn_ref[i].astype(F32)
    oattn_ref[:, 0:128] = total[0:5]
    oattn_ref[:, 128:256] = total[5:10]
    oattn_ref[:, 256:320] = total[10:15, 0:64]
    conv = conv_ref[...].astype(F32).reshape(32 * NF, 128)
    oconv_ref[:, 0:128] = conv[0:180]
    oconv_ref[:, 128:256] = conv[192:372]
    oconv_ref[0:90, 256:320] = conv[384:474, 0:64]
    oconv_ref[90:180, 256:320] = conv[384:474, 64:128]


def finish(gi, attn, conv):
    vm = pl.BlockSpec(memory_space=pltpu.VMEM)
    return pl.pallas_call(
        finish_kernel,
        out_shape=(
            jax.ShapeDtypeStruct((2, W, W, C), BF16),
            jax.ShapeDtypeStruct((5, C), F32),
            jax.ShapeDtypeStruct((180, C), F32),
        ),
        in_specs=[vm] * 3,
        out_specs=(vm, vm, vm),
        name="finish",
    )(gi, attn, conv)


def body(clip_latents, out_grad, box_mask, attn_weights, conv_weights, time_bias):
    got = block(clip_latents[0], out_grad[0], box_mask[0], attn_weights.T, conv_weights.T, time_bias)
    out, oattn, oconv = finish(*got)
    return out[None], oattn, oconv


def solution(mesh):
    in_specs = (
        P("dp", "frame", "height", None, None),
        P("dp", "frame", "height", None, None),
        P("dp", "frame", "height", None),
        P(),
        P(),
        P(),
    )
    out_specs = (
        P("dp", "frame", "height", None, None),
        P(("frame", "height", "dp"), None),
        P(("height", "dp"), None),
    )
    return jax.shard_map(body, mesh=mesh, in_specs=in_specs, out_specs=out_specs, check_vma=False)
```

```python
import jax
import jax.numpy as jnp
from jax import lax
from jax.experimental import pallas as pl
from jax.experimental.pallas import tpu as pltpu
from jax.sharding import PartitionSpec as P

F32 = jnp.float32
BF16 = jnp.bfloat16
GROUND_BIAS = 2.0
NF, NH, ND = 16, 8, 2
C = 320
PK = 640
HEADS = 5
T = 32
W = 16
ROWS = T * W
BLK = 128
NB = ROWS // BLK
NEG = -1e30
TOKENS = 2 * 32 * 128 * 16
GRAD_SCALE = float(TOKENS) ** -0.5
SCALING = 0.125


def peer(**where):
    return dict(device_id=where, device_id_type=pl.DeviceIdType.MESH)


def nn(a, b):
    return lax.dot_general(a, b, (((1,), (0,)), ((), ())), preferred_element_type=F32)


def nt(a, b):
    return lax.dot_general(a, b, (((1,), (1,)), ((), ())), preferred_element_type=F32)


def tn(a, b):
    return lax.dot_general(a, b, (((0,), (0,)), ((), ())), preferred_element_type=F32)


def pixel_major(src, tr, store):
    for s in range(5):
        tr[s, 0 : NF * W, :] = src[:, :, 128 * s : 128 * s + 128].reshape(NF * W, 128).astype(F32)
    for p in range(W):
        for e in range(2):
            for s in range(2):
                store(p, e, 128 * s, 128, tr[2 * e + s, pl.ds(p, NF, stride=W), :].astype(BF16))
            store(p, e, 256, 64, tr[4, pl.ds(p, NF, stride=W), :][:, 64 * e : 64 * e + 64].astype(BF16))


def pack(src, dst):
    for e in range(2):
        dst[:, :, 256 * e : 256 * e + 256] = src[e, :, :, 0:256]
    dst[:, :, 512:640] = jnp.concatenate([src[0, :, :, 256:320], src[1, :, :, 256:320]], axis=-1)


ORDER = (1, 15, 8, 2, 14, 7, 9, 3, 13, 6, 10, 4, 12, 5, 11)
SLABS = ((0, 128, (0, 1)), (128, 128, (2, 3)), (256, 64, (4,)))


def block_kernel(
    x_hbm, dy_hbm, mark_ref, wat_ref, wct_ref, tb_ref,
    out_ref, attn_cr, conv_dr,
    x_ref, dy_ref, xs, ys, ms, mt, xt, dy0, dyu, dyd, wa, wc,
    tr, xp, dyp, q_s, k_s, v_s, o_s, pr, bias_s, y1_s, a_t, da_s, g_s, do_s, dq_s, dk_s, dv_s, x_t, o_t, cf,
    gi_s, attn_f, attn_l, conv_l, conv_a, attn_a, conv_1, attn_1, conv_b, attn_b, conv_f, conv_c, conv_cr, conv_d, attn_g, attn_w, attn_c,
    mss, msr, xss, xsr, dss, dsr, hs, hr, gs, gr, pa, pb, cs, cr, as_, ar, c2s, c2r, c3s, c3r, a2s, a2r, lsem,
):
    f = lax.axis_index("frame")
    h = lax.axis_index("height")
    d = lax.axis_index("dp")
    other = 1 - d
    me = h * ND + d
    lin = h * NF + f
    prev = lax.rem(lin + NF * NH - 1, NF * NH)
    nxt = lax.rem(lin + 1, NF * NH)

    def remote(src, dst, ss, rs, **where):
        cp = pltpu.make_async_remote_copy(src_ref=src, dst_ref=dst, send_sem=ss, recv_sem=rs, **peer(**where))
        cp.start()
        return cp

    inx = pltpu.make_async_copy(x_hbm, x_ref, lsem.at[6])
    iny = pltpu.make_async_copy(dy_hbm, dy_ref, lsem.at[7])
    inx.start()
    iny.start()
    barrier = pltpu.get_barrier_semaphore()
    for k in range(1, NF):
        pl.semaphore_signal(barrier, inc=1, **peer(frame=lax.rem(f + k, NF)))
    for k in range(1, NH * ND):
        q = lax.rem(me + k, NH * ND)
        pl.semaphore_signal(barrier, inc=1, **peer(height=q // ND, dp=lax.rem(q, ND)))

    @pl.when(f == 0)
    def _():
        pl.semaphore_signal(barrier, inc=1, **peer(frame=lax.rem(prev, NF), height=prev // NF))

    @pl.when(f == NF - 1)
    def _():
        pl.semaphore_signal(barrier, inc=1, **peer(frame=lax.rem(nxt, NF), height=nxt // NF))

    lwa = pltpu.make_async_copy(wat_ref, wa, lsem.at[0])
    lwc = pltpu.make_async_copy(wct_ref, wc, lsem.at[1])
    lwa.start()
    lwc.start()

    inx.wait()
    pack(x_ref, xs)
    ms[:, 0, :] = jnp.zeros((NF, 128), F32)
    ms[:, 0, 0 : 2 * W] = jnp.concatenate([mark_ref[0], mark_ref[1]], axis=-1).astype(F32)
    iny.wait()
    pack(dy_ref, ys)

    edge = jnp.where(jnp.logical_or(f == 0, f == NF - 1), 1, 0)
    pl.semaphore_wait(barrier, NF + NH * ND - 2 + edge)

    xc, mc, dc = [], [], []
    for k in range(1, NF):
        p = lax.rem(f + k, NF)
        mc.append(remote(ms.at[p], mt.at[f], mss.at[k], msr.at[k], frame=p))
        xc.append(remote(xs.at[p], xt.at[f], xss.at[k], xsr.at[k], frame=p))
    for k in range(1, NF):
        p = lax.rem(f + k, NF)
        dc.append(remote(ys.at[p], dy0.at[f], dss.at[k], dsr.at[k], frame=p))
    lx = pltpu.make_async_copy(xs.at[f], xt.at[f], lsem.at[2])
    ld = pltpu.make_async_copy(ys.at[f], dy0.at[f], lsem.at[3])
    lm = pltpu.make_async_copy(ms.at[f], mt.at[f], lsem.at[5])
    lx.start()
    ld.start()
    lm.start()
    fwd = []

    def forward(k):
        part = lax.rem(f + NF - k, NF)
        up = remote(dy0.at[part], dyd.at[part], hs.at[0, k], hr.at[0, k], frame=lax.rem(prev, NF), height=prev // NF)
        down = remote(dy0.at[part], dyu.at[part], hs.at[1, k], hr.at[1, k], frame=lax.rem(nxt, NF), height=nxt // NF)
        fwd.append((up, down))

    ld.wait()
    forward(0)
    waiting = list(ORDER)

    def forward_next():
        if waiting:
            k = waiting.pop(0)
            dc[k - 1].wait_recv()
            forward(k)

    ri = lax.broadcasted_iota(jnp.int32, (BLK, BLK), 0) // T
    ci = lax.broadcasted_iota(jnp.int32, (BLK, BLK), 1) // T
    tq = lax.broadcasted_iota(jnp.int32, (T, T), 0)
    tu = lax.broadcasted_iota(jnp.int32, (T, T), 1)
    turn = jnp.where(tu == 2 * (tq & (NF - 1)) + (tq >> 4), 1.0, 0.0)

    def exact(left, right, dim):
        return lax.dot_general(
            left, right, (((1,), (dim,)), ((), ())), precision=lax.Precision.HIGHEST, preferred_element_type=F32
        )

    for hd in range(HEADS):
        one = exact(exact(turn, tb_ref[hd], 0), turn, 1)
        wide = jnp.concatenate([one] * 4, axis=1)
        full = jnp.concatenate([wide] * 4, axis=0)
        bias_s[hd] = jnp.where(ri == ci, full, NEG)
    conv_l[...] = jnp.zeros_like(conv_l)
    attn_f[...] = jnp.zeros_like(attn_f)
    attn_w[...] = jnp.zeros_like(attn_w)
    zero = jnp.zeros((T, C), BF16)
    for r in range(3):
        dyp[r, 0:T, :] = zero
        dyp[r, (W + 1) * T :, :] = zero
    lane = lax.broadcasted_iota(jnp.int32, (BLK, 128), 1)
    low = lane < 64
    ones = jnp.full((8, 128), GROUND_BIAS, BF16)

    def only(val, i, w):
        if w == 64:
            return val
        keep = low if i == 0 else jnp.logical_not(low)
        return jnp.where(keep, val, jnp.zeros_like(val))

    def pick(parts, w):
        if w == 64:
            return parts[0]
        return jnp.where(low, parts[0], parts[1])

    lwa.wait()
    lx.wait()
    lm.wait()
    for k in ORDER:
        mc[k - 1].wait_recv()
        xc[k - 1].wait_recv()

    def put_x(p, e, s, w, val):
        xp[p * T + e * NF : p * T + (e + 1) * NF, s : s + w] = val

    pixel_major(xt, tr, put_x)
    x = xp[...]
    marks_all = jnp.concatenate([mt[:, 0, :]] * 8, axis=0)
    row_b = lax.broadcasted_iota(jnp.int32, (BLK, 128), 0)
    home = ((row_b >> 4) & 1) * W + (row_b >> 5)
    q_s[...] = nt(x, wa[:, 0:C]).astype(BF16)
    k_s[...] = nt(x, wa[:, C : 2 * C]).astype(BF16)
    v_s[...] = nt(x, wa[:, 2 * C : 3 * C]).astype(BF16)

    for b in range(NB):
        rows = slice(b * BLK, (b + 1) * BLK)
        marks = jnp.where(lane == home + 4 * b, marks_all, 0.0).astype(BF16)
        key_bias = nt(ones, marks)[0:1, :]
        for s, w, heads in SLABS:
            ls = slice(s, s + w)
            qb, kb, vb = q_s[rows, ls], k_s[rows, ls], v_s[rows, ls]
            outs = []
            for i, hd in enumerate(heads):
                sc = nt(only(qb, i, w), kb) * SCALING + bias_s[hd] + key_bias
                e = jnp.exp(sc - jnp.max(sc, axis=-1, keepdims=True))
                pf = e / jnp.sum(e, axis=-1, keepdims=True)
                pr[b, hd] = pf
                outs.append(nn(pf.astype(BF16), vb))
            o_s[rows, ls] = pick(outs, w).astype(BF16)
            forward_next()
    while waiting:
        forward_next()

    y1 = (x.astype(F32) + nt(o_s[...], wa[:, 3 * C :])).astype(BF16)
    y1_s[...] = y1
    yf = y1.astype(F32)
    act = yf / (1.0 + jnp.exp(-yf))
    a_t[...] = act.T.astype(BF16)

    def place_row(r, src, keep):
        def put(p, e, s, w, val):
            if keep is not None:
                val = jnp.where(keep, val, jnp.zeros_like(val))
            at = (p + 1) * T + e * NF
            dyp[r, at : at + NF, s : s + w] = val

        pixel_major(src, tr, put)

    def shifted(c, r):
        return dyp[r, (2 - c) * T : (2 - c) * T + ROWS, :]

    def kernel_taps(r):
        for c in range(3):
            tap = 3 * r + c
            cf[tap * C : (tap + 1) * C, :] = nn(a_t[...], shifted(c, r)) * GRAD_SCALE

    def data_taps(r, first):
        for c in range(3):
            tap = 3 * r + c
            part = nn(shifted(c, r), wc[:, tap * C : (tap + 1) * C])
            da_s[...] = part if first else da_s[...] + part
            first = False

    def halve(first, last, i):
        for k in range(ND * first, ND * last):
            at = 180 * k
            to = conv_l.at[k // ND, k % ND]
            to[0:180, :] = cf[at : at + 180, 0:128].astype(BF16)
            to[192:372, :] = cf[at : at + 180, 128:256].astype(BF16)
            ends = [cf[at : at + 90, 256:320], cf[at + 90 : at + 180, 256:320]]
            to[384:474, :] = jnp.concatenate(ends, axis=-1).astype(BF16)
        part = pl.ds(first, last - first)
        return remote(conv_l.at[part, other], conv_a.at[part], pa.at[i], pb.at[i], dp=other)

    cc = []
    for k in range(1, NH):
        cc.append(
            pltpu.make_async_remote_copy(
                src_ref=conv_1.at[lax.rem(h + k, NH)],
                dst_ref=conv_b.at[k],
                send_sem=cs.at[k],
                recv_sem=cr.at[k],
                **peer(height=lax.rem(h + k, NH)),
            )
        )

    def spread(first, last):
        for j in range(first, last):
            conv_1[j] = (conv_l[j, d].astype(F32) + conv_a[j].astype(F32)).astype(BF16)
        for k in range(1, NH):
            p = lax.rem(h + k, NH)

            @pl.when(jnp.logical_and(p >= first, p < last))
            def _(k=k):
                cc[k - 1].start()

    place_row(1, dy0, None)
    kernel_taps(1)
    ca = halve(3, 5, 0)
    lwc.wait()
    data_taps(1, True)
    ca.wait_recv()
    spread(3, 5)
    rr = lax.broadcasted_iota(jnp.int32, (C, C), 0)
    cc_ = lax.broadcasted_iota(jnp.int32, (C, C), 1)
    mm = (rr * 3277) >> 16
    rem = rr - 20 * mm
    cf_ = (rem * 13108) >> 16
    perm = jnp.where(cc_ == 80 * cf_ + 5 * mm + (rem - 5 * cf_), 1.0, 0.0).astype(BF16)
    x_t[...] = nt(perm, x).astype(BF16)
    o_t[...] = nt(perm, o_s[...]).astype(BF16)
    for up, _ in fwd:
        up.wait_recv()
    place_row(0, dyd, lin < NF * NH - 1)
    kernel_taps(0)
    cb = halve(0, 3, 2)
    for _, down in fwd:
        down.wait_recv()
    place_row(2, dyu, lin > 0)
    kernel_taps(2)
    cd = halve(5, NH, 3)
    data_taps(0, False)
    cb.wait_recv()
    spread(0, 3)
    data_taps(2, False)
    cd.wait_recv()
    spread(5, NH)

    yf = y1_s[...].astype(F32)
    sig = 1.0 / (1.0 + jnp.exp(-yf))
    slope = sig * (1.0 + yf * (1.0 - sig))
    g = (dyp[1, T : T + ROWS, :].astype(F32) + slope * da_s[...]).astype(BF16)
    g_s[...] = g
    do_s[...] = nn(g, wa[:, 3 * C :]).astype(BF16)

    def attn_term(j, left, right):
        term = nn(left[...], right[...]) * GRAD_SCALE
        for m in range(NH * ND):
            piece = term[20 * m : 20 * m + 20, :]
            attn_f[m, 20 * j : 20 * j + 20, :] = piece[:, 0:128]
            attn_f[m, 80 + 20 * j : 100 + 20 * j, :] = piece[:, 128:256]
            attn_f[m, 160 + 10 * j : 170 + 10 * j, :] = jnp.concatenate([piece[0:10, 256:], piece[10:20, 256:]], axis=-1)

    attn_term(3, o_t, g_s)

    for b in range(NB):
        rows = slice(b * BLK, (b + 1) * BLK)
        for s, w, heads in SLABS:
            ls = slice(s, s + w)
            qb, kb, vb, db = q_s[rows, ls], k_s[rows, ls], v_s[rows, ls], do_s[rows, ls]
            dqs, dks, dvs = [], [], []
            for i, hd in enumerate(heads):
                pf = pr[b, hd]
                dp = nt(only(db, i, w), vb)
                dsc = (pf * (dp - jnp.sum(pf * dp, axis=-1, keepdims=True))).astype(BF16)
                dqs.append(nn(dsc, kb))
                dks.append(tn(dsc, qb))
                dvs.append(tn(pf.astype(BF16), db))
            dq_s[rows, ls] = (pick(dqs, w) * SCALING).astype(BF16)
            dk_s[rows, ls] = (pick(dks, w) * SCALING).astype(BF16)
            dv_s[rows, ls] = pick(dvs, w).astype(BF16)

    for j, right in enumerate((dq_s, dk_s, dv_s)):
        attn_term(j, x_t, right)
    for m in range(NH * ND):
        attn_l[m // ND, m % ND] = attn_f[m].astype(BF16)
    aa = remote(attn_l.at[:, other], attn_a, pa.at[1], pb.at[1], dp=other)

    total = conv_1[h].astype(F32)
    for k in range(1, NH):
        cc[k - 1].wait_recv()
        total = total + conv_b[k].astype(F32)
    conv_f[0:480, :] = total
    conv_f[480:512, :] = jnp.zeros((32, 128), F32)
    for j in range(NF):
        conv_c[j] = conv_f[32 * j : 32 * j + 32, :].astype(BF16)
    c2 = []
    for k in range(1, NF):
        p = lax.rem(f + k, NF)
        c2.append(remote(conv_c.at[p], conv_cr.at[k], c2s.at[k], c2r.at[k], frame=p))

    dx = nn(dq_s[...], wa[:, 0:C]) + nn(dk_s[...], wa[:, C : 2 * C]) + nn(dv_s[...], wa[:, 2 * C : 3 * C])
    gi = g_s[...].astype(F32) + dx.astype(BF16).astype(F32)
    for s in range(2):
        tr[s] = gi[:, 128 * s : 128 * s + 128]
    tr[2, :, 0:64] = gi[:, 256:320]
    for t in range(NF):
        for e in range(2):
            for s in range(2):
                at = 256 * e + 128 * s
                gi_s[t, :, at : at + 128] = tr[s, pl.ds(e * NF + t, W, stride=T), :].astype(BF16)
        ends = [tr[2, pl.ds(e * NF + t, W, stride=T), :][:, 0:64] for e in range(2)]
        gi_s[t, :, 512:640] = jnp.concatenate(ends, axis=-1).astype(BF16)
    gic = []
    for k in range(1, NF):
        p = lax.rem(f + k, NF)
        gic.append(remote(gi_s.at[p], out_ref.at[f], gs.at[k], gr.at[k], frame=p))
    own = pltpu.make_async_copy(gi_s.at[f], out_ref.at[f], lsem.at[4])
    own.start()

    aa.wait_recv()
    for j in range(NH):
        attn_1[j] = (attn_l[j, d].astype(F32) + attn_a[j].astype(F32)).astype(BF16)
    ac = []
    for k in range(1, NH):
        p = lax.rem(h + k, NH)
        ac.append(remote(attn_1.at[p], attn_b.at[k], as_.at[k], ar.at[k], height=p))

    total = attn_1[h].astype(F32)
    for k in range(1, NH):
        ac[k - 1].wait_recv()
        total = total + attn_b[k].astype(F32)
    attn_g[...] = total
    for j in range(NF):
        at = 160 + 10 * (j // 4) + 5 * (j % 2)
        to = 64 * (j % 4 // 2)
        attn_w[j, 0:5, :] = attn_g[5 * j : 5 * j + 5, :]
        attn_w[j, 5:10, :] = attn_g[80 + 5 * j : 85 + 5 * j, :]
        attn_w[j, 10:15, 0:64] = attn_g[at : at + 5, to : to + 64]
    for j in range(NF):
        attn_c[j] = attn_w[j].astype(BF16)
    a2 = []
    for k in range(1, NF):
        p = lax.rem(f + k, NF)
        a2.append(remote(attn_c.at[p], attn_cr.at[k], a2s.at[k], a2r.at[k], frame=p))
    attn_cr[0] = attn_c[f]

    total = conv_c[f].astype(F32)
    for k in range(1, NF):
        c2[k - 1].wait_recv()
        total = total + conv_cr[k].astype(F32)
    conv_d[...] = total.astype(BF16)
    c3 = []
    for k in range(1, NF):
        p = lax.rem(f + k, NF)
        c3.append(remote(conv_d, conv_dr.at[f], c3s.at[k], c3r.at[k], frame=p))
    conv_dr[f] = total.astype(BF16)

    own.wait()
    for cp in a2 + c3 + gic:
        cp.wait_recv()
    for cp in mc + xc + dc + [ca, cb, cd, aa] + gic + cc + ac + a2 + c2 + c3:
        cp.wait_send()
    for up, down in fwd:
        up.wait_send()
        down.wait_send()


def block(x, dy, marks, wat, wct, tb):
    vm = pl.BlockSpec(memory_space=pltpu.VMEM)
    anyw = pl.BlockSpec(memory_space=pl.ANY)
    v = pltpu.VMEM
    dma = pltpu.SemaphoreType.DMA
    tok = v((ROWS, C), BF16)
    row = v((NF, W, PK), BF16)
    mark = v((NF, 1, 128), F32)
    return pl.pallas_call(
        block_kernel,
        out_shape=(
            jax.ShapeDtypeStruct((W, W, PK), BF16),
            jax.ShapeDtypeStruct((NF, 16, 128), BF16),
            jax.ShapeDtypeStruct((NF, 32, 128), BF16),
        ),
        in_specs=[anyw, anyw, vm, anyw, anyw, vm],
        out_specs=(vm, vm, vm),
        scratch_shapes=[
            v((2, W, W, C), BF16), v((2, W, W, C), BF16), row, row, mark, mark, row, row, row, row, v((C, 4 * C), BF16), v((C, 9 * C), BF16),
            v((5, ROWS, 128), F32), v((ROWS, C), BF16), v((3, ROWS + 2 * T, C), BF16),
            tok, tok, tok, tok,
            v((NB, HEADS, BLK, BLK), F32), v((HEADS, BLK, BLK), F32),
            tok, v((C, ROWS), BF16), v((ROWS, C), F32), tok, tok, tok, tok, tok,
            v((C, ROWS), BF16), v((C, ROWS), BF16), v((9 * C, C), F32),
            row, v((NH * ND, 208, 128), F32), v((NH, ND, 208, 128), BF16), v((NH, ND, 480, 128), BF16),
            v((NH, 480, 128), BF16), v((NH, 208, 128), BF16), v((NH, 480, 128), BF16), v((NH, 208, 128), BF16),
            v((NH, 480, 128), BF16), v((NH, 208, 128), BF16),
            v((512, 128), F32), v((NF, 32, 128), BF16), v((NF, 32, 128), BF16), v((32, 128), BF16),
            v((208, 128), F32), v((NF, 16, 128), F32), v((NF, 16, 128), BF16),
            dma((NF,)), dma((NF,)), dma((NF,)), dma((NF,)), dma((NF,)), dma((NF,)), dma((2, NF)), dma((2, NF)),
            dma((NF,)), dma((NF,)), dma((4,)), dma((4,)), dma((NH,)), dma((NH,)), dma((NH,)), dma((NH,)),
            dma((NF,)), dma((NF,)), dma((NF,)), dma((NF,)), dma((NF,)), dma((NF,)), dma((8,)),
        ],
        compiler_params=pltpu.CompilerParams(collective_id=0, has_side_effects=True),
        name="block_backward",
    )(x, dy, marks, wat, wct, tb)


def finish_kernel(gi_ref, attn_ref, conv_ref, out_ref, oattn_ref, oconv_ref):
    for e in range(2):
        out_ref[e, :, :, 0:256] = gi_ref[:, :, 256 * e : 256 * e + 256]
        out_ref[e, :, :, 256:320] = gi_ref[:, :, 512 + 64 * e : 576 + 64 * e]
    total = attn_ref[0].astype(F32)
    for i in range(1, NF):
        total = total + attn_ref[i].astype(F32)
    oattn_ref[:, 0:128] = total[0:5]
    oattn_ref[:, 128:256] = total[5:10]
    oattn_ref[:, 256:320] = total[10:15, 0:64]
    conv = conv_ref[...].astype(F32).reshape(32 * NF, 128)
    oconv_ref[:, 0:128] = conv[0:180]
    oconv_ref[:, 128:256] = conv[192:372]
    oconv_ref[0:90, 256:320] = conv[384:474, 0:64]
    oconv_ref[90:180, 256:320] = conv[384:474, 64:128]


def finish(gi, attn, conv):
    vm = pl.BlockSpec(memory_space=pltpu.VMEM)
    return pl.pallas_call(
        finish_kernel,
        out_shape=(
            jax.ShapeDtypeStruct((2, W, W, C), BF16),
            jax.ShapeDtypeStruct((5, C), F32),
            jax.ShapeDtypeStruct((180, C), F32),
        ),
        in_specs=[vm] * 3,
        out_specs=(vm, vm, vm),
        name="finish",
    )(gi, attn, conv)


def body(clip_latents, out_grad, box_mask, attn_weights, conv_weights, time_bias):
    got = block(clip_latents[0], out_grad[0], box_mask[0], attn_weights.T, conv_weights.T, time_bias)
    out, oattn, oconv = finish(*got)
    return out[None], oattn, oconv


def solution(mesh):
    in_specs = (
        P("dp", "frame", "height", None, None),
        P("dp", "frame", "height", None, None),
        P("dp", "frame", "height", None),
        P(),
        P(),
        P(),
    )
    out_specs = (
        P("dp", "frame", "height", None, None),
        P(("frame", "height", "dp"), None),
        P(("height", "dp"), None),
    )
    return jax.shard_map(body, mesh=mesh, in_specs=in_specs, out_specs=out_specs, check_vma=False)
```

```python
import jax
import jax.numpy as jnp
from jax import lax
from jax.experimental import pallas as pl
from jax.experimental.pallas import tpu as pltpu
from jax.sharding import PartitionSpec as P

F32 = jnp.float32
BF16 = jnp.bfloat16
GROUND_BIAS = 2.0
NF, NH, ND = 16, 8, 2
C = 320
PK = 640
HEADS = 5
T = 32
W = 16
ROWS = T * W
BLK = 128
NB = ROWS // BLK
NEG = -1e30
TOKENS = 2 * 32 * 128 * 16
GRAD_SCALE = float(TOKENS) ** -0.5
SCALING = 0.125


def peer(**where):
    return dict(device_id=where, device_id_type=pl.DeviceIdType.MESH)


def nn(a, b):
    return lax.dot_general(a, b, (((1,), (0,)), ((), ())), preferred_element_type=F32)


def nt(a, b):
    return lax.dot_general(a, b, (((1,), (1,)), ((), ())), preferred_element_type=F32)


def tn(a, b):
    return lax.dot_general(a, b, (((0,), (0,)), ((), ())), preferred_element_type=F32)


def pixel_major(src, tr, store):
    for s in range(5):
        tr[s, 0 : NF * W, :] = src[:, :, 128 * s : 128 * s + 128].reshape(NF * W, 128).astype(F32)
    for p in range(W):
        for e in range(2):
            for s in range(2):
                store(p, e, 128 * s, 128, tr[2 * e + s, pl.ds(p, NF, stride=W), :].astype(BF16))
            store(p, e, 256, 64, tr[4, pl.ds(p, NF, stride=W), :][:, 64 * e : 64 * e + 64].astype(BF16))


def pack(src, dst):
    for e in range(2):
        dst[:, :, 256 * e : 256 * e + 256] = src[e, :, :, 0:256]
    dst[:, :, 512:640] = jnp.concatenate([src[0, :, :, 256:320], src[1, :, :, 256:320]], axis=-1)


ORDER = (1, 15, 8, 2, 14, 7, 9, 3, 13, 6, 10, 4, 12, 5, 11)
SLABS = ((0, 128, (0, 1)), (128, 128, (2, 3)), (256, 64, (4,)))


def block_kernel(
    x_hbm, dy_hbm, mark_ref, wat_ref, wct_ref, tb_ref,
    out_ref, attn_cr, conv_dr,
    x_ref, dy_ref, xs, ys, ms, mt, xt, dy0, dyu, dyd, wa, wc,
    tr, xp, dyp, q_s, k_s, v_s, o_s, pr, bias_s, y1_s, a_t, da_s, g_s, do_s, dq_s, dk_s, dv_s, x_t, o_t, cf,
    gi_s, attn_f, attn_l, conv_l, conv_a, attn_a, conv_1, attn_1, conv_b, attn_b, conv_f, conv_c, conv_cr, conv_d, attn_g, attn_w, attn_c,
    mss, msr, xss, xsr, dss, dsr, hs, hr, gs, gr, pa, pb, cs, cr, as_, ar, c2s, c2r, c3s, c3r, a2s, a2r, lsem,
):
    f = lax.axis_index("frame")
    h = lax.axis_index("height")
    d = lax.axis_index("dp")
    other = 1 - d
    me = h * ND + d
    lin = h * NF + f
    prev = lax.rem(lin + NF * NH - 1, NF * NH)
    nxt = lax.rem(lin + 1, NF * NH)

    def remote(src, dst, ss, rs, **where):
        cp = pltpu.make_async_remote_copy(src_ref=src, dst_ref=dst, send_sem=ss, recv_sem=rs, **peer(**where))
        cp.start()
        return cp

    inx = pltpu.make_async_copy(x_hbm, x_ref, lsem.at[6])
    iny = pltpu.make_async_copy(dy_hbm, dy_ref, lsem.at[7])
    inx.start()
    iny.start()
    barrier = pltpu.get_barrier_semaphore()
    for k in range(1, NF):
        pl.semaphore_signal(barrier, inc=1, **peer(frame=lax.rem(f + k, NF)))
    for k in range(1, NH * ND):
        q = lax.rem(me + k, NH * ND)
        pl.semaphore_signal(barrier, inc=1, **peer(height=q // ND, dp=lax.rem(q, ND)))

    @pl.when(f == 0)
    def _():
        pl.semaphore_signal(barrier, inc=1, **peer(frame=lax.rem(prev, NF), height=prev // NF))

    @pl.when(f == NF - 1)
    def _():
        pl.semaphore_signal(barrier, inc=1, **peer(frame=lax.rem(nxt, NF), height=nxt // NF))

    lwa = pltpu.make_async_copy(wat_ref, wa, lsem.at[0])
    lwc = pltpu.make_async_copy(wct_ref, wc, lsem.at[1])
    lwa.start()
    lwc.start()

    inx.wait()
    pack(x_ref, xs)
    ms[:, 0, :] = jnp.zeros((NF, 128), F32)
    ms[:, 0, 0 : 2 * W] = jnp.concatenate([mark_ref[0], mark_ref[1]], axis=-1).astype(F32)
    iny.wait()
    pack(dy_ref, ys)

    edge = jnp.where(jnp.logical_or(f == 0, f == NF - 1), 1, 0)
    pl.semaphore_wait(barrier, NF + NH * ND - 2 + edge)

    xc, mc, dc = [], [], []
    for k in range(1, NF):
        p = lax.rem(f + k, NF)
        mc.append(remote(ms.at[p], mt.at[f], mss.at[k], msr.at[k], frame=p))
        xc.append(remote(xs.at[p], xt.at[f], xss.at[k], xsr.at[k], frame=p))
    for k in range(1, NF):
        p = lax.rem(f + k, NF)
        dc.append(remote(ys.at[p], dy0.at[f], dss.at[k], dsr.at[k], frame=p))
    lx = pltpu.make_async_copy(xs.at[f], xt.at[f], lsem.at[2])
    ld = pltpu.make_async_copy(ys.at[f], dy0.at[f], lsem.at[3])
    lm = pltpu.make_async_copy(ms.at[f], mt.at[f], lsem.at[5])
    lx.start()
    ld.start()
    lm.start()
    fwd = []

    def forward(k):
        part = lax.rem(f + NF - k, NF)
        up = remote(dy0.at[part], dyd.at[part], hs.at[0, k], hr.at[0, k], frame=lax.rem(prev, NF), height=prev // NF)
        down = remote(dy0.at[part], dyu.at[part], hs.at[1, k], hr.at[1, k], frame=lax.rem(nxt, NF), height=nxt // NF)
        fwd.append((up, down))

    ld.wait()
    forward(0)
    waiting = list(ORDER)

    def forward_next():
        if waiting:
            k = waiting.pop(0)
            dc[k - 1].wait_recv()
            forward(k)

    ri = lax.broadcasted_iota(jnp.int32, (BLK, BLK), 0) // T
    ci = lax.broadcasted_iota(jnp.int32, (BLK, BLK), 1) // T
    tq = lax.broadcasted_iota(jnp.int32, (T, T), 0)
    tu = lax.broadcasted_iota(jnp.int32, (T, T), 1)
    turn = jnp.where(tu == 2 * (tq & (NF - 1)) + (tq >> 4), 1.0, 0.0)

    def exact(left, right, dim):
        return lax.dot_general(
            left, right, (((1,), (dim,)), ((), ())), precision=lax.Precision.HIGHEST, preferred_element_type=F32
        )

    for hd in range(HEADS):
        one = exact(exact(turn, tb_ref[hd], 0), turn, 1)
        wide = jnp.concatenate([one] * 4, axis=1)
        full = jnp.concatenate([wide] * 4, axis=0)
        bias_s[hd] = jnp.where(ri == ci, full, NEG)
    conv_l[...] = jnp.zeros_like(conv_l)
    attn_f[...] = jnp.zeros_like(attn_f)
    attn_w[...] = jnp.zeros_like(attn_w)
    zero = jnp.zeros((T, C), BF16)
    for r in range(3):
        dyp[r, 0:T, :] = zero
        dyp[r, (W + 1) * T :, :] = zero
    lane = lax.broadcasted_iota(jnp.int32, (BLK, 128), 1)
    low = lane < 64
    ones = jnp.full((8, 128), GROUND_BIAS, BF16)

    def only(val, i, w):
        if w == 64:
            return val
        keep = low if i == 0 else jnp.logical_not(low)
        return jnp.where(keep, val, jnp.zeros_like(val))

    def pick(parts, w):
        if w == 64:
            return parts[0]
        return jnp.where(low, parts[0], parts[1])

    lwa.wait()
    lx.wait()
    lm.wait()
    for k in ORDER:
        mc[k - 1].wait_recv()
        xc[k - 1].wait_recv()

    def put_x(p, e, s, w, val):
        xp[p * T + e * NF : p * T + (e + 1) * NF, s : s + w] = val

    pixel_major(xt, tr, put_x)
    x = xp[...]
    marks_all = jnp.concatenate([mt[:, 0, :]] * 8, axis=0)
    row_b = lax.broadcasted_iota(jnp.int32, (BLK, 128), 0)
    home = ((row_b >> 4) & 1) * W + (row_b >> 5)
    q_s[...] = nt(x, wa[:, 0:C]).astype(BF16)
    k_s[...] = nt(x, wa[:, C : 2 * C]).astype(BF16)
    v_s[...] = nt(x, wa[:, 2 * C : 3 * C]).astype(BF16)

    for b in range(NB):
        rows = slice(b * BLK, (b + 1) * BLK)
        marks = jnp.where(lane == home + 4 * b, marks_all, 0.0).astype(BF16)
        key_bias = nt(ones, marks)[0:1, :]
        for s, w, heads in SLABS:
            ls = slice(s, s + w)
            qb, kb, vb = q_s[rows, ls], k_s[rows, ls], v_s[rows, ls]
            outs = []
            for i, hd in enumerate(heads):
                sc = nt(only(qb, i, w), kb) * SCALING + bias_s[hd] + key_bias
                e = jnp.exp(sc - jnp.max(sc, axis=-1, keepdims=True))
                pf = e / jnp.sum(e, axis=-1, keepdims=True)
                pr[b, hd] = pf
                outs.append(nn(pf.astype(BF16), vb))
            o_s[rows, ls] = pick(outs, w).astype(BF16)
            forward_next()
    while waiting:
        forward_next()

    y1 = (x.astype(F32) + nt(o_s[...], wa[:, 3 * C :])).astype(BF16)
    y1_s[...] = y1
    yf = y1.astype(F32)
    act = yf / (1.0 + jnp.exp(-yf))
    a_t[...] = act.T.astype(BF16)

    def place_row(r, src, keep):
        def put(p, e, s, w, val):
            if keep is not None:
                val = jnp.where(keep, val, jnp.zeros_like(val))
            at = (p + 1) * T + e * NF
            dyp[r, at : at + NF, s : s + w] = val

        pixel_major(src, tr, put)

    def shifted(c, r):
        return dyp[r, (2 - c) * T : (2 - c) * T + ROWS, :]

    def kernel_taps(r):
        for c in range(3):
            tap = 3 * r + c
            cf[tap * C : (tap + 1) * C, :] = nn(a_t[...], shifted(c, r)) * GRAD_SCALE

    def data_taps(r, first):
        for c in range(3):
            tap = 3 * r + c
            part = nn(shifted(c, r), wc[:, tap * C : (tap + 1) * C])
            da_s[...] = part if first else da_s[...] + part
            first = False

    def halve(first, last, i):
        for k in range(ND * first, ND * last):
            at = 180 * k
            to = conv_l.at[k // ND, k % ND]
            to[0:180, :] = cf[at : at + 180, 0:128].astype(BF16)
            to[192:372, :] = cf[at : at + 180, 128:256].astype(BF16)
            ends = [cf[at : at + 90, 256:320], cf[at + 90 : at + 180, 256:320]]
            to[384:474, :] = jnp.concatenate(ends, axis=-1).astype(BF16)
        part = pl.ds(first, last - first)
        return remote(conv_l.at[part, other], conv_a.at[part], pa.at[i], pb.at[i], dp=other)

    cc = []
    for k in range(1, NH):
        cc.append(
            pltpu.make_async_remote_copy(
                src_ref=conv_1.at[lax.rem(h + k, NH)],
                dst_ref=conv_b.at[k],
                send_sem=cs.at[k],
                recv_sem=cr.at[k],
                **peer(height=lax.rem(h + k, NH)),
            )
        )

    def spread(first, last):
        for j in range(first, last):
            conv_1[j] = (conv_l[j, d].astype(F32) + conv_a[j].astype(F32)).astype(BF16)
        for k in range(1, NH):
            p = lax.rem(h + k, NH)

            @pl.when(jnp.logical_and(p >= first, p < last))
            def _(k=k):
                cc[k - 1].start()

    place_row(1, dy0, None)
    kernel_taps(1)
    ca = halve(3, 5, 0)
    lwc.wait()
    data_taps(1, True)
    ca.wait_recv()
    spread(3, 5)
    rr = lax.broadcasted_iota(jnp.int32, (C, C), 0)
    cc_ = lax.broadcasted_iota(jnp.int32, (C, C), 1)
    mm = (rr * 3277) >> 16
    rem = rr - 20 * mm
    cf_ = (rem * 13108) >> 16
    perm = jnp.where(cc_ == 80 * cf_ + 5 * mm + (rem - 5 * cf_), 1.0, 0.0).astype(BF16)
    x_t[...] = nt(perm, x).astype(BF16)
    o_t[...] = nt(perm, o_s[...]).astype(BF16)
    for up, _ in fwd:
        up.wait_recv()
    place_row(0, dyd, lin < NF * NH - 1)
    kernel_taps(0)
    cb = halve(0, 3, 2)
    for _, down in fwd:
        down.wait_recv()
    place_row(2, dyu, lin > 0)
    kernel_taps(2)
    cd = halve(5, NH, 3)
    data_taps(0, False)
    cb.wait_recv()
    spread(0, 3)
    data_taps(2, False)
    cd.wait_recv()
    spread(5, NH)

    yf = y1_s[...].astype(F32)
    sig = 1.0 / (1.0 + jnp.exp(-yf))
    slope = sig * (1.0 + yf * (1.0 - sig))
    g = (dyp[1, T : T + ROWS, :].astype(F32) + slope * da_s[...]).astype(BF16)
    g_s[...] = g
    do_s[...] = nn(g, wa[:, 3 * C :]).astype(BF16)

    def attn_term(j, left, right):
        term = nn(left[...], right[...]) * GRAD_SCALE
        for m in range(NH * ND):
            piece = term[20 * m : 20 * m + 20, :]
            attn_f[m, 20 * j : 20 * j + 20, :] = piece[:, 0:128]
            attn_f[m, 80 + 20 * j : 100 + 20 * j, :] = piece[:, 128:256]
            attn_f[m, 160 + 10 * j : 170 + 10 * j, :] = jnp.concatenate([piece[0:10, 256:], piece[10:20, 256:]], axis=-1)

    attn_term(3, o_t, g_s)

    for b in range(NB):
        rows = slice(b * BLK, (b + 1) * BLK)
        for s, w, heads in SLABS:
            ls = slice(s, s + w)
            qb, kb, vb, db = q_s[rows, ls], k_s[rows, ls], v_s[rows, ls], do_s[rows, ls]
            dqs, dks, dvs = [], [], []
            for i, hd in enumerate(heads):
                pf = pr[b, hd]
                dp = nt(only(db, i, w), vb)
                dsc = (pf * (dp - jnp.sum(pf * dp, axis=-1, keepdims=True))).astype(BF16)
                dqs.append(nn(dsc, kb))
                dks.append(tn(dsc, qb))
                dvs.append(tn(pf.astype(BF16), db))
            dq_s[rows, ls] = (pick(dqs, w) * SCALING).astype(BF16)
            dk_s[rows, ls] = (pick(dks, w) * SCALING).astype(BF16)
            dv_s[rows, ls] = pick(dvs, w).astype(BF16)

    dx = nn(dq_s[...], wa[:, 0:C]) + nn(dk_s[...], wa[:, C : 2 * C]) + nn(dv_s[...], wa[:, 2 * C : 3 * C])
    gi = g_s[...].astype(F32) + dx.astype(BF16).astype(F32)
    for s in range(2):
        tr[s] = gi[:, 128 * s : 128 * s + 128]
    tr[2, :, 0:64] = gi[:, 256:320]
    for t in range(NF):
        for e in range(2):
            for s in range(2):
                at = 256 * e + 128 * s
                gi_s[t, :, at : at + 128] = tr[s, pl.ds(e * NF + t, W, stride=T), :].astype(BF16)
        ends = [tr[2, pl.ds(e * NF + t, W, stride=T), :][:, 0:64] for e in range(2)]
        gi_s[t, :, 512:640] = jnp.concatenate(ends, axis=-1).astype(BF16)
    gic = []
    for k in range(1, NF):
        p = lax.rem(f + k, NF)
        gic.append(remote(gi_s.at[p], out_ref.at[f], gs.at[k], gr.at[k], frame=p))
    own = pltpu.make_async_copy(gi_s.at[f], out_ref.at[f], lsem.at[4])
    own.start()

    for j, right in enumerate((dq_s, dk_s, dv_s)):
        attn_term(j, x_t, right)
    for m in range(NH * ND):
        attn_l[m // ND, m % ND] = attn_f[m].astype(BF16)
    aa = remote(attn_l.at[:, other], attn_a, pa.at[1], pb.at[1], dp=other)

    total = conv_1[h].astype(F32)
    for k in range(1, NH):
        cc[k - 1].wait_recv()
        total = total + conv_b[k].astype(F32)
    conv_f[0:480, :] = total
    conv_f[480:512, :] = jnp.zeros((32, 128), F32)
    for j in range(NF):
        conv_c[j] = conv_f[32 * j : 32 * j + 32, :].astype(BF16)
    c2 = []
    for k in range(1, NF):
        p = lax.rem(f + k, NF)
        c2.append(remote(conv_c.at[p], conv_cr.at[k], c2s.at[k], c2r.at[k], frame=p))

    aa.wait_recv()
    for j in range(NH):
        attn_1[j] = (attn_l[j, d].astype(F32) + attn_a[j].astype(F32)).astype(BF16)
    ac = []
    for k in range(1, NH):
        p = lax.rem(h + k, NH)
        ac.append(remote(attn_1.at[p], attn_b.at[k], as_.at[k], ar.at[k], height=p))

    total = attn_1[h].astype(F32)
    for k in range(1, NH):
        ac[k - 1].wait_recv()
        total = total + attn_b[k].astype(F32)
    attn_g[...] = total
    for j in range(NF):
        at = 160 + 10 * (j // 4) + 5 * (j % 2)
        to = 64 * (j % 4 // 2)
        attn_w[j, 0:5, :] = attn_g[5 * j : 5 * j + 5, :]
        attn_w[j, 5:10, :] = attn_g[80 + 5 * j : 85 + 5 * j, :]
        attn_w[j, 10:15, 0:64] = attn_g[at : at + 5, to : to + 64]
    for j in range(NF):
        attn_c[j] = attn_w[j].astype(BF16)
    a2 = []
    for k in range(1, NF):
        p = lax.rem(f + k, NF)
        a2.append(remote(attn_c.at[p], attn_cr.at[k], a2s.at[k], a2r.at[k], frame=p))
    attn_cr[0] = attn_c[f]

    total = conv_c[f].astype(F32)
    for k in range(1, NF):
        c2[k - 1].wait_recv()
        total = total + conv_cr[k].astype(F32)
    conv_d[...] = total.astype(BF16)
    c3 = []
    for k in range(1, NF):
        p = lax.rem(f + k, NF)
        c3.append(remote(conv_d, conv_dr.at[f], c3s.at[k], c3r.at[k], frame=p))
    conv_dr[f] = total.astype(BF16)

    own.wait()
    for cp in a2 + c3 + gic:
        cp.wait_recv()
    for cp in mc + xc + dc + [ca, cb, cd, aa] + gic + cc + ac + a2 + c2 + c3:
        cp.wait_send()
    for up, down in fwd:
        up.wait_send()
        down.wait_send()


def block(x, dy, marks, wat, wct, tb):
    vm = pl.BlockSpec(memory_space=pltpu.VMEM)
    anyw = pl.BlockSpec(memory_space=pl.ANY)
    v = pltpu.VMEM
    dma = pltpu.SemaphoreType.DMA
    tok = v((ROWS, C), BF16)
    row = v((NF, W, PK), BF16)
    mark = v((NF, 1, 128), F32)
    return pl.pallas_call(
        block_kernel,
        out_shape=(
            jax.ShapeDtypeStruct((W, W, PK), BF16),
            jax.ShapeDtypeStruct((NF, 16, 128), BF16),
            jax.ShapeDtypeStruct((NF, 32, 128), BF16),
        ),
        in_specs=[anyw, anyw, vm, anyw, anyw, vm],
        out_specs=(vm, vm, vm),
        scratch_shapes=[
            v((2, W, W, C), BF16), v((2, W, W, C), BF16), row, row, mark, mark, row, row, row, row, v((C, 4 * C), BF16), v((C, 9 * C), BF16),
            v((5, ROWS, 128), F32), v((ROWS, C), BF16), v((3, ROWS + 2 * T, C), BF16),
            tok, tok, tok, tok,
            v((NB, HEADS, BLK, BLK), F32), v((HEADS, BLK, BLK), F32),
            tok, v((C, ROWS), BF16), v((ROWS, C), F32), tok, tok, tok, tok, tok,
            v((C, ROWS), BF16), v((C, ROWS), BF16), v((9 * C, C), F32),
            row, v((NH * ND, 208, 128), F32), v((NH, ND, 208, 128), BF16), v((NH, ND, 480, 128), BF16),
            v((NH, 480, 128), BF16), v((NH, 208, 128), BF16), v((NH, 480, 128), BF16), v((NH, 208, 128), BF16),
            v((NH, 480, 128), BF16), v((NH, 208, 128), BF16),
            v((512, 128), F32), v((NF, 32, 128), BF16), v((NF, 32, 128), BF16), v((32, 128), BF16),
            v((208, 128), F32), v((NF, 16, 128), F32), v((NF, 16, 128), BF16),
            dma((NF,)), dma((NF,)), dma((NF,)), dma((NF,)), dma((NF,)), dma((NF,)), dma((2, NF)), dma((2, NF)),
            dma((NF,)), dma((NF,)), dma((4,)), dma((4,)), dma((NH,)), dma((NH,)), dma((NH,)), dma((NH,)),
            dma((NF,)), dma((NF,)), dma((NF,)), dma((NF,)), dma((NF,)), dma((NF,)), dma((8,)),
        ],
        compiler_params=pltpu.CompilerParams(collective_id=0, has_side_effects=True),
        name="block_backward",
    )(x, dy, marks, wat, wct, tb)


def finish_kernel(gi_ref, attn_ref, conv_ref, out_ref, oattn_ref, oconv_ref):
    for e in range(2):
        out_ref[e, :, :, 0:256] = gi_ref[:, :, 256 * e : 256 * e + 256]
        out_ref[e, :, :, 256:320] = gi_ref[:, :, 512 + 64 * e : 576 + 64 * e]
    total = attn_ref[0].astype(F32)
    for i in range(1, NF):
        total = total + attn_ref[i].astype(F32)
    oattn_ref[:, 0:128] = total[0:5]
    oattn_ref[:, 128:256] = total[5:10]
    oattn_ref[:, 256:320] = total[10:15, 0:64]
    conv = conv_ref[...].astype(F32).reshape(32 * NF, 128)
    oconv_ref[:, 0:128] = conv[0:180]
    oconv_ref[:, 128:256] = conv[192:372]
    oconv_ref[0:90, 256:320] = conv[384:474, 0:64]
    oconv_ref[90:180, 256:320] = conv[384:474, 64:128]


def finish(gi, attn, conv):
    vm = pl.BlockSpec(memory_space=pltpu.VMEM)
    return pl.pallas_call(
        finish_kernel,
        out_shape=(
            jax.ShapeDtypeStruct((2, W, W, C), BF16),
            jax.ShapeDtypeStruct((5, C), F32),
            jax.ShapeDtypeStruct((180, C), F32),
        ),
        in_specs=[vm] * 3,
        out_specs=(vm, vm, vm),
        name="finish",
    )(gi, attn, conv)


def body(clip_latents, out_grad, box_mask, attn_weights, conv_weights, time_bias):
    got = block(clip_latents[0], out_grad[0], box_mask[0], attn_weights.T, conv_weights.T, time_bias)
    out, oattn, oconv = finish(*got)
    return out[None], oattn, oconv


def solution(mesh):
    in_specs = (
        P("dp", "frame", "height", None, None),
        P("dp", "frame", "height", None, None),
        P("dp", "frame", "height", None),
        P(),
        P(),
        P(),
    )
    out_specs = (
        P("dp", "frame", "height", None, None),
        P(("frame", "height", "dp"), None),
        P(("height", "dp"), None),
    )
    return jax.shard_map(body, mesh=mesh, in_specs=in_specs, out_specs=out_specs, check_vma=False)
```
